256 devices in a mesh: dp: 8 (over y, z_hi), fsdp: 32 (over z_lo, x, core).
Axes of the slice: x: 4, y: 4, z: 8 (z_hi: 2, z_lo: 4; z = z_hi * 4 + z_lo), core: 2. Of those that a mesh axis runs over, the one named last changes fastest.
Arguments:
- tokens: bfloat16 [1024, 3072], P('dp'), may hold values from -6 to 6
- cotangent: bfloat16 [1024, 3072], P('dp'), may hold values from -6 to 6
- routes: int32 [1024, 2], P('dp'), may hold values from 0 to 7, all different within a row; in each aligned block of 128 rows (0 to 127, 128 to 255, ...) at most 48 rows name the same one
- router_weight: float32 [1024, 2], P('dp'), may hold values from 0.25 to 1
- w_gate: bfloat16 [8, 3072, 8192], P('dp', None, 'fsdp'), may hold values from -0.109375 to 0.109375
- w_up: bfloat16 [8, 3072, 8192], P('dp', None, 'fsdp'), may hold values from -0.109375 to 0.109375
- w_down: bfloat16 [8, 8192, 3072], P('dp', 'fsdp'), may hold values from -0.0625 to 0.0625
Outputs:
- output: bfloat16 [1024, 3072], P('dp')
- input_grad: bfloat16 [1024, 3072], P('dp')
- grad_gate: bfloat16 [8, 3072, 8192], P('dp', None, 'fsdp')
- grad_up: bfloat16 [8, 3072, 8192], P('dp', None, 'fsdp')
- grad_down: bfloat16 [8, 8192, 3072], P('dp', 'fsdp')
The draws below stay inside these ranges and needn't reach their ends.
Inputs may be any that keep to these rules, and one draw needn't show every extreme that they name: `routes`: the two experts of a token differ. In the 128 rows of one batch no expert is named by more than 48 rows, a bound that some block reaches in some batches.
All inputs are finite; a program needn't handle non-finite values.
Results may differ from the reference program's by a relative error of at most 0.025.
Values may be sent and summed in bfloat16 or wider, within the bound.
A program may use at most 128 MiB of HBM per device.

```python
import math
import jax
import jax.numpy as jnp
import numpy as np
from jax import lax

D = 3072
F = 8192
TOK_DEV = 128
EXPERTS = 8
CAP = 48
TOKENS = 1024
N_DP = 8
N_FSDP = 32


def levels(rng, shape, shards, low, top_value):
    level = 1.0
    for dim, parts in shards:
        heights = jax.random.uniform(jax.random.fold_in(jax.random.fold_in(rng, 6), dim), (parts,), jnp.float32, low / len(shards), top_value / len(shards))
        level = level * jnp.repeat(jnp.exp(heights), shape[dim] // parts).reshape((-1,) + (1,) * (len(shape) - 1 - dim))
    return level


def assign_block(stream_key, own, number, rows, count, top, limit, lean):
    sequence = jax.random.permutation(stream_key, count)
    crowded, common = portions_of(count, rows * top, limit, lean, True), portions_of(count, rows * top, limit, lean, False)
    places = jnp.arange(count)

    def named(lengths, offset_by):
        used = int((lengths > 0).sum())
        fixed = max(1, used // 4)
        passed = fixed + (places - fixed + offset_by * (used - fixed)) % max(1, count - fixed)
        return jnp.zeros((count,), jnp.int32).at[sequence[jnp.where(places < fixed, places, passed)]].set(jnp.asarray(lengths, jnp.int32))

    lengths = jnp.where(number % 4 == 0, named(crowded, number // 4), named(common, number - number // 4 - 1))
    mixed = jax.random.permutation(jax.random.fold_in(own, 3), count)
    source_of, sink = mixed[0:count // 2 * 2:2], mixed[1:count // 2 * 2:2]
    room = jnp.minimum(lengths[source_of] - 1, limit - lengths[sink]) // 2
    room = jnp.where((source_of == sequence[0]) | (sink == sequence[0]) | (lengths[sink] == 0), 0, jnp.maximum(room, 0))
    passed = jax.random.randint(jax.random.fold_in(own, 4), (count // 2,), 0, 1 << 20) % (room + 1)
    lengths = lengths.at[source_of].add(-passed).at[sink].add(passed)
    labels = jnp.searchsorted(jnp.cumsum(lengths), jnp.arange(rows * top), side="right").astype(jnp.int32)
    grid = labels.reshape(top, rows).T
    grid = grid[jax.random.permutation(jax.random.fold_in(own, 1), rows)]
    offset_by = jax.random.randint(jax.random.fold_in(own, 2), (rows, 1), 0, top)
    return jnp.take_along_axis(grid, (jnp.arange(top)[None, :] + offset_by) % top, axis=1)


def portions_of(number_of, total, bound, skew, full):
    portions = [(1 << 20) // math.isqrt(grade ** skew) + 1 for grade in range(1, number_of + 1)]
    largest = bound if full else min(bound, max(-(-total // number_of), total * portions[0] // sum(portions)))
    least = 1 if total - largest >= number_of - 1 else 0
    given, surplus = [largest] + [least] * (number_of - 1), total - largest - least * (number_of - 1)
    while surplus > 0:
        candidates = [i for i in range(1, number_of) if given[i] < largest] or [i for i in range(1, number_of) if given[i] < bound]
        whole, budget = sum([portions[i] for i in candidates]), surplus
        for i in candidates:
            extra = min(bound - given[i], max(1, budget * portions[i] // whole), surplus)
            given[i] = given[i] + extra
            surplus = surplus - extra
    return np.array(given)


def bell_draw(key, extent, width, bound, split=(), kind=jnp.bfloat16):
    gain = levels(key, extent, split, -0.22, 0.18) if split else 1.0
    entries = jax.random.normal(key, extent, jnp.float32) * width * gain
    return jnp.minimum(jnp.maximum(entries, -bound), bound).astype(kind)


def setup_inputs(seed: int = 0) -> dict:
    seeds = jax.random.split(jax.random.key(seed), 8)
    tokens = bell_draw(seeds[0], (TOKENS, D), 1.0, 6.0, ((0, 8),))
    cotangent = bell_draw(seeds[1], (TOKENS, D), 1.0, 6.0, ((0, 8),))
    routes_keys = jax.random.split(jax.random.fold_in(seeds[2], 1), TOKENS // TOK_DEV)
    routes_turns = jax.random.permutation(jax.random.fold_in(seeds[2], 3), TOKENS // TOK_DEV)
    routes = jax.vmap(lambda own, number: assign_block(jax.random.fold_in(seeds[2], 2), own, number, TOK_DEV, N_DP, 2, CAP, 1))(routes_keys, routes_turns).reshape((TOKENS, 2))
    router_weight = jnp.clip(0.25 + 0.75 * jax.random.uniform(seeds[3], (TOKENS, 2), jnp.float32) ** levels(seeds[3], (TOKENS, 2), ((0, 8),), -0.2, 0.2), 0.25, 1.0)
    w_gate = bell_draw(seeds[4], (EXPERTS, D, F), D ** -0.5, 0.109375, ((0, 8), (2, 32)))
    w_up = bell_draw(seeds[5], (EXPERTS, D, F), D ** -0.5, 0.109375, ((0, 8), (2, 32)))
    w_down = bell_draw(seeds[6], (EXPERTS, F, D), F ** -0.5, 0.0625, ((0, 8), (1, 32)))
    return dict(tokens=tokens, cotangent=cotangent, routes=routes, router_weight=router_weight, w_gate=w_gate, w_up=w_up, w_down=w_down)


def slot_tables(routes, router_weight):
    expert_ids = jnp.arange(N_DP, dtype=jnp.int32)
    hit_table = (routes[..., None] == expert_ids).astype(jnp.int32)
    per_token = jnp.sum(hit_table, axis=2)
    before = jnp.cumsum(per_token, axis=1) - per_token
    slot_of = jnp.sum(hit_table * before[:, :, None, :], axis=3)
    slot_ids = jnp.arange(CAP, dtype=jnp.int32)
    placed = hit_table[..., None] * (slot_of[..., None, None] == slot_ids).astype(jnp.int32)
    picked = jnp.sum(placed, axis=2).astype(jnp.float32)
    weighted = jnp.sum(placed.astype(jnp.float32) * router_weight[..., None, None], axis=2)
    return picked, weighted


def expert_pass(operands):
    slot_x, slot_dy, gate_w, up_w, down_w = operands
    gate_pre = jnp.dot(slot_x, gate_w, preferred_element_type=jnp.float32)
    up_pre = jnp.dot(slot_x, up_w, preferred_element_type=jnp.float32)
    sigma = jax.nn.sigmoid(gate_pre)
    active = gate_pre * sigma
    hidden = (active * up_pre).astype(jnp.bfloat16)
    hidden_dy = jnp.dot(slot_dy, down_w.T, preferred_element_type=jnp.float32)
    gate_dy = (hidden_dy * up_pre * sigma * (1.0 + gate_pre * (1.0 - sigma))).astype(jnp.bfloat16)
    up_dy = (hidden_dy * active).astype(jnp.bfloat16)
    grad_down = jnp.dot(hidden.T, slot_dy, preferred_element_type=jnp.float32).astype(jnp.bfloat16)
    grad_gate = jnp.dot(slot_x.T, gate_dy, preferred_element_type=jnp.float32).astype(jnp.bfloat16)
    grad_up = jnp.dot(slot_x.T, up_dy, preferred_element_type=jnp.float32).astype(jnp.bfloat16)
    block_width = F // N_FSDP

    def one_block(carry, index):
        start = (index * block_width).astype(jnp.int32)
        hidden_part = lax.dynamic_slice_in_dim(hidden, start, block_width, 1)
        gate_part = lax.dynamic_slice_in_dim(gate_dy, start, block_width, 1)
        up_part = lax.dynamic_slice_in_dim(up_dy, start, block_width, 1)
        down_rows = lax.dynamic_slice_in_dim(down_w, start, block_width, 0)
        gate_cols = lax.dynamic_slice_in_dim(gate_w, start, block_width, 1)
        up_cols = lax.dynamic_slice_in_dim(up_w, start, block_width, 1)
        out_term = jnp.dot(hidden_part, down_rows, preferred_element_type=jnp.float32).astype(jnp.bfloat16)
        out_term = lax.optimization_barrier(out_term)
        back_term = (jnp.dot(gate_part, gate_cols.T, preferred_element_type=jnp.float32)
                     + jnp.dot(up_part, up_cols.T, preferred_element_type=jnp.float32)).astype(jnp.bfloat16)
        back_term = lax.optimization_barrier(back_term)
        return (carry[0] + out_term.astype(jnp.float32), carry[1] + back_term.astype(jnp.float32)), None

    zeros = jnp.zeros((slot_x.shape[0], D), jnp.float32)
    totals, unused = lax.scan(one_block, (zeros, zeros), jnp.arange(N_FSDP, dtype=jnp.int32))
    return totals[0].astype(jnp.bfloat16), totals[1].astype(jnp.bfloat16), grad_gate, grad_up, grad_down


def reference(tokens, cotangent, routes, router_weight, w_gate, w_up, w_down):
    blocks = TOKENS // TOK_DEV
    highest = lax.Precision.HIGHEST
    inputs = tokens.reshape(blocks, TOK_DEV, D).astype(jnp.float32)
    grads_in = cotangent.reshape(blocks, TOK_DEV, D).astype(jnp.float32)
    picked, weighted = slot_tables(routes.reshape(blocks, TOK_DEV, 2), router_weight.reshape(blocks, TOK_DEV, 2))
    slot_x = jnp.einsum('btec,btd->ebcd', picked, inputs, precision=highest).astype(jnp.bfloat16)
    slot_dy = jnp.einsum('btec,btd->ebcd', weighted, grads_in, precision=highest).astype(jnp.bfloat16)
    slot_x = slot_x.reshape(N_DP, blocks * CAP, D)
    slot_dy = slot_dy.reshape(N_DP, blocks * CAP, D)
    slot_out, slot_dx, grad_gate, grad_up, grad_down = lax.map(expert_pass, (slot_x, slot_dy, w_gate, w_up, w_down))
    slot_out = slot_out.reshape(N_DP, blocks, CAP, D).astype(jnp.float32)
    slot_dx = slot_dx.reshape(N_DP, blocks, CAP, D).astype(jnp.float32)
    output = jnp.einsum('btec,ebcd->btd', weighted, slot_out, precision=highest).astype(jnp.bfloat16)
    input_grad = jnp.einsum('btec,ebcd->btd', picked, slot_dx, precision=highest).astype(jnp.bfloat16)
    return (output.reshape(TOKENS, D), input_grad.reshape(TOKENS, D), grad_gate, grad_up, grad_down)
```

```python
import functools

import jax
import jax.numpy as jnp
from jax import lax
from jax.experimental import pallas as pl
from jax.experimental.pallas import tpu as pltpu
from jax.sharding import PartitionSpec as P

MESH = pl.DeviceIdType.MESH
NY, NZH, NZ, NX, NC = 4, 2, 4, 4, 2
BF, F32 = jnp.bfloat16, jnp.float32
TRAIL = (((1,), (1,)), ((), ()))
LEAD = (((0,), (0,)), ((), ()))


class Dims:
    def __init__(self, tok, feat, hid):
        self.tok, self.feat, self.hid = tok, feat, hid
        self.cap = tok * 3 // 8
        self.grp = NY * self.cap
        self.quart = feat // NX
        self.half = self.quart // 2
        self.tile = self.quart // 6


def experts_kernel(
    dims,
    send, first_pick, second_pick, pick_w, gate_hbm, up_hbm, down_hbm,
    out_hbm, gg_hbm, gu_hbm, gd_hbm,
    arr, wg, wu, wd, hid, gdy, udy, tt, dd, rl1, rr1, rl2, rr2, yy, zr, ww, uu, outs, gg, gu, gd,
    ss, rs, ls,
):
    cap, grp, quart, half, tile = dims.cap, dims.grp, dims.quart, dims.half, dims.tile
    dp, fs = lax.axis_index("dp"), lax.axis_index("fsdp")
    y, zh = dp // 2, dp % 2
    z, x, k = fs // 8, (fs // 2) % 4, fs % 2
    other = 1 - k

    def dev(yy_, zh_, z_, x_, k_):
        return (yy_ * 2 + zh_, (z_ * 4 + x_) * 2 + k_)

    def up_y(d):
        return (y + d) % 4

    right, left = dev(y, zh, z, (x + 1) % 4, k), dev(y, zh, z, (x + 3) % 4, k)
    sibling = dev(y, zh, z, x, other)

    used = [0]
    pending = []

    def fresh():
        used[0] += 1
        return used[0] - 1

    def copy(i, src, dst, to):
        return pltpu.make_async_remote_copy(
            src_ref=src, dst_ref=dst, send_sem=ss.at[i], recv_sem=rs.at[i],
            device_id=to, device_id_type=MESH,
        )

    def push(i, src, dst, to):
        c = copy(i, src, dst, to)
        c.start()
        pending.append(c)

    def got(i, region):
        copy(i, region, region, sibling).wait_recv()

    def qcols(q, off=0, width=None):
        return pl.ds(pl.multiple_of(q * quart + off, 128), quart if width is None else width)

    def rows_of(b):
        return pl.ds(pl.multiple_of(b * cap, 16), cap)

    loads = [
        pltpu.make_async_copy(s, d, ls.at[n])
        for n, (s, d) in enumerate(((gate_hbm, wg), (up_hbm, wu), (down_hbm, wd)))
    ]
    for c in loads:
        c.start()

    barrier = pltpu.get_barrier_semaphore()
    partners = [right, left, sibling]
    for d in range(1, 4):
        partners.append(dev(y, zh, (z + d) % 4, x, k))
    for d in range(4):
        if d:
            partners.append(dev(up_y(d), zh, z, x, k))
        partners.append(dev(up_y(d), 1 - zh, z, x, k))
    for p in partners:
        pl.semaphore_signal(barrier, inc=1, device_id=p, device_id_type=MESH)
    pl.semaphore_wait(barrier, len(partners))

    zc = 1 - zh
    cross_ids, same_ids, both_ids = {}, {}, {}
    for d in (0, 1, 3, 2):
        cross_ids[d] = fresh()
        push(
            cross_ids[d],
            send.at[zc, rows_of(up_y(d)), qcols(x)],
            arr.at[k, zh, rows_of(y), qcols(x)],
            dev(up_y(d), zc, z, x, k),
        )
    for d in (1, 3, 2):
        same_ids[d] = fresh()
        push(
            same_ids[d],
            send.at[zh, rows_of(up_y(d))],
            arr.at[k, zh, rows_of(y)],
            dev(up_y(d), zh, z, x, k),
        )
    for g in range(2):
        for d in range(4):
            both_ids[g, d] = fresh()
    push(both_ids[0, 0], send.at[zh, rows_of(y)], arr.at[k, zh, rows_of(y)], sibling)
    arr[k, zh, rows_of(y)] = send[zh, rows_of(y)]
    for d in (1, 3, 2):
        block = arr.at[k, zh, rows_of(up_y(4 - d))]
        got(same_ids[d], block)
        push(both_ids[0, d], block, block, sibling)
    ring = {}
    for d in (0, 1, 3, 2):
        rows = rows_of(up_y(4 - d))
        mine = arr.at[k, zc, rows, qcols(x)]
        got(cross_ids[d], mine)
        ring[d] = [fresh() for _ in range(4)]
        push(ring[d][0], mine, mine, right)
        push(ring[d][1], mine, mine, left)

    def first_stage(g):
        zg = zh if g == 0 else zc
        gate_pre = jnp.dot(arr[0, zg], wg[...], preferred_element_type=F32)
        up_pre = jnp.dot(arr[0, zg], wu[...], preferred_element_type=F32)
        hidden_dy = lax.dot_general(arr[1, zg], wd[...], TRAIL, preferred_element_type=F32)
        sigma = jax.nn.sigmoid(gate_pre)
        active = gate_pre * sigma
        hid[zg] = (active * up_pre).astype(BF)
        gdy[zg] = (hidden_dy * up_pre * sigma * (1.0 + gate_pre * (1.0 - sigma))).astype(BF)
        udy[zg] = (hidden_dy * active).astype(BF)

    quarters = [(x + 2) % 4, (x + 1) % 4, (x + 3) % 4, x]
    swap_ids = {(g, n): fresh() for g in range(2) for n in range(4)}

    def second_stage(g):
        zg = zh if g == 0 else zc
        width = quart // 3
        for n, q in enumerate(quarters):

            def body(c, carry, q=q):
                at = pl.ds(pl.multiple_of(q * quart + c * width, 128), width)
                tt[g, 0, :, at] = jnp.dot(
                    hid[zg], wd[:, at], preferred_element_type=F32
                ).astype(BF)
                tt[g, 1, :, at] = (
                    lax.dot_general(gdy[zg], wg[at, :], TRAIL, preferred_element_type=F32)
                    + lax.dot_general(udy[zg], wu[at, :], TRAIL, preferred_element_type=F32)
                ).astype(BF)
                return carry

            lax.fori_loop(0, 3, body, 0)
            push(swap_ids[g, n], tt.at[g, other, :, qcols(q)], dd.at[g, :, qcols(q)], sibling)

    def plus(a, b):
        return (a.astype(F32) + b.astype(F32)).astype(BF)

    hop_ids = {(g, n): fresh() for g in range(2) for n in range(6)}

    def chip_sum(g, n):
        q = quarters[n]
        got(swap_ids[g, n], dd.at[g, :, qcols(q)])
        tt[g, k, :, qcols(q)] = plus(tt[g, k, :, qcols(q)], dd[g, :, qcols(q)])

    def hop_one(g):
        chip_sum(g, 0)
        far = quarters[0]
        push(hop_ids[g, 0], tt.at[g, k, :, qcols(far, 0, half)], rl1.at[g], right)
        push(hop_ids[g, 1], tt.at[g, k, :, qcols(far, half, half)], rr1.at[g], left)
        chip_sum(g, 1)
        push(
            hop_ids[g, 2], tt.at[g, k, :, qcols(quarters[1], half, half)],
            rl2.at[g, :, pl.ds(half, half)], right,
        )
        chip_sum(g, 2)
        push(
            hop_ids[g, 3], tt.at[g, k, :, qcols(quarters[2], 0, half)],
            rr2.at[g, :, pl.ds(0, half)], left,
        )
        chip_sum(g, 3)

    def hop_two(g):
        got(hop_ids[g, 0], rl1.at[g])
        at = qcols(quarters[1], 0, half)
        tt[g, k, :, at] = plus(tt[g, k, :, at], rl1[g])
        push(hop_ids[g, 4], tt.at[g, k, :, at], rl2.at[g, :, pl.ds(0, half)], right)
        got(hop_ids[g, 1], rr1.at[g])
        at = qcols(quarters[2], half, half)
        tt[g, k, :, at] = plus(tt[g, k, :, at], rr1[g])
        push(hop_ids[g, 5], tt.at[g, k, :, at], rr2.at[g, :, pl.ds(half, half)], left)

    def head(zz):
        return (3 * zz + 1 - k) // 2

    def pair(zz):
        return (zz + k) % 2 == 0

    def tcols(t, base=0):
        return pl.ds(pl.multiple_of(base + t * tile, 128), tile)

    tile_ids = {(g, d, s): fresh() for g in range(2) for d in range(1, 4) for s in range(2)}

    def along_z(g):
        for n in (2, 3, 4, 5):
            region = (rl2 if n in (2, 4) else rr2).at[
                g, :, pl.ds(half if n in (2, 5) else 0, half)
            ]
            got(hop_ids[g, n], region)
        yy[g] = (
            tt[g, k, :, qcols(x)].astype(F32) + rl2[g].astype(F32) + rr2[g].astype(F32)
        ).astype(BF)
        for d in range(1, 4):
            zz = (z + d) % 4
            to = dev(y, zh, zz, x, k)
            push(tile_ids[g, d, 0], yy.at[g, :, tcols(head(zz))], zr.at[g, d - 1, 0], to)

            @pl.when(pair(zz))
            def _(d=d, zz=zz, to=to):
                copy(
                    tile_ids[g, d, 1], yy.at[g, :, tcols(head(zz) + 1)], zr.at[g, d - 1, 1], to
                ).start()

    back_ids = {(g, d): fresh() for g in range(2) for d in range(4)}

    def home(g):
        zg = zh if g == 0 else zc

        def summed(s):
            total = yy[g, :, tcols(head(z) + s)].astype(F32)
            for d in range(1, 4):
                total = total + zr[g, d - 1, s].astype(F32)
            ww[g, :, pl.ds(s * tile, tile)] = total.astype(BF)

        for d in range(1, 4):
            got(tile_ids[g, d, 0], zr.at[g, d - 1, 0])
        summed(0)

        @pl.when(pair(z))
        def _():
            for d in range(1, 4):
                got(tile_ids[g, d, 1], zr.at[g, d - 1, 1])
            summed(1)

        @pl.when(jnp.logical_not(pair(z)))
        def _():
            ww[g, :, pl.ds(tile, tile)] = jnp.zeros((grp, tile), BF)

        for d in (1, 3, 2, 0):
            if g == 0 and d == 0:
                uu[zh, rows_of(y)] = ww[0, rows_of(y)]
            else:
                push(
                    back_ids[g, d], ww.at[g, rows_of(up_y(d))], uu.at[zh, rows_of(y)],
                    dev(up_y(d), zg, z, x, k),
                )

    grad_copies = []

    def weight_grads():
        width = 256
        rows = 2 * grp

        def body(c, carry):
            at = pl.ds(pl.multiple_of(c * width, 128), width)
            xs = arr[0, :, :, at].reshape(rows, width)
            ys = arr[1, :, :, at].reshape(rows, width)
            hidden = hid[...].reshape(rows, dims.hid)
            gg[at, :] = lax.dot_general(
                xs, gdy[...].reshape(rows, dims.hid), LEAD, preferred_element_type=F32
            ).astype(BF)
            gu[at, :] = lax.dot_general(
                xs, udy[...].reshape(rows, dims.hid), LEAD, preferred_element_type=F32
            ).astype(BF)
            gd[:, at] = lax.dot_general(
                hidden, ys, LEAD, preferred_element_type=F32
            ).astype(BF)
            return carry

        lax.fori_loop(0, dims.feat // width, body, 0)
        for n, (s, d) in enumerate(((gg, gg_hbm), (gu, gu_hbm), (gd, gd_hbm))):
            c = pltpu.make_async_copy(s, d, ls.at[3 + n])
            c.start()
            grad_copies.append(c)

    for c in loads:
        c.wait()
    for d in range(4):
        got(both_ids[0, d], arr.at[other, zh, rows_of(up_y(4 - d) if d else y)])
    first_stage(0)
    for d in (0, 1, 3, 2):
        rows = rows_of(up_y(4 - d))
        from_left = arr.at[k, zc, rows, qcols((x + 3) % 4)]
        from_right = arr.at[k, zc, rows, qcols((x + 1) % 4)]
        got(ring[d][0], from_left)
        got(ring[d][1], from_right)
        near = arr.at[k, zc, rows, qcols((x + 3) % 4, 0, half)]
        push(ring[d][2], near, near, right)
        near = arr.at[k, zc, rows, qcols((x + 1) % 4, half, half)]
        push(ring[d][3], near, near, left)
    second_stage(0)
    for d in (0, 1, 3, 2):
        rows = rows_of(up_y(4 - d))
        got(ring[d][2], arr.at[k, zc, rows, qcols((x + 2) % 4, 0, half)])
        got(ring[d][3], arr.at[k, zc, rows, qcols((x + 2) % 4, half, half)])
        block = arr.at[k, zc, rows]
        push(both_ids[1, d], block, block, sibling)
    hop_one(0)
    for d in range(4):
        got(both_ids[1, d], arr.at[other, zc, rows_of(up_y(4 - d) if d else y)])
    first_stage(1)
    second_stage(1)
    hop_two(0)
    hop_one(1)
    weight_grads()
    along_z(0)
    hop_two(1)
    home(0)
    along_z(1)
    home(1)

    for g in range(2):
        zg = zh if g == 0 else zc
        for d in range(4):
            if g or d:
                got(back_ids[g, d], uu.at[zg, rows_of(up_y(4 - d) if d else y)])
    slots = uu[...].reshape(2 * grp, 2 * tile)
    mixed = (
        pick_w[:, 0:1] * jnp.dot(first_pick[...], slots, preferred_element_type=F32)
        + pick_w[:, 1:2] * jnp.dot(second_pick[...], slots, preferred_element_type=F32)
    ).astype(BF)
    base = x * quart
    outs[k, :, tcols(head(z), base)] = mixed[:, :tile]

    @pl.when(pair(z))
    def _():
        outs[k, :, tcols(head(z) + 1, base)] = mixed[:, tile:]

    last_ids = {(d, s): fresh() for d in range(1, 4) for s in range(2)}
    for d in range(1, 4):
        mine = outs.at[k, :, tcols(head(z), base)]
        to = dev(y, zh, (z + d) % 4, x, k)
        push(last_ids[d, 0], mine, mine, to)

        @pl.when(pair(z))
        def _(d=d, to=to):
            second = outs.at[k, :, tcols(head(z) + 1, base)]
            copy(last_ids[d, 1], second, second, to).start()

    for d in range(1, 4):
        zz = (z + 4 - d) % 4
        got(last_ids[d, 0], outs.at[k, :, tcols(head(zz), base)])

        @pl.when(pair(zz))
        def _(d=d, zz=zz):
            got(last_ids[d, 1], outs.at[k, :, tcols(head(zz) + 1, base)])

    turn = [fresh() for _ in range(4)]
    share = [fresh() for _ in range(4)]
    mine = outs.at[k, :, qcols(x)]
    push(turn[0], mine, mine, right)
    push(turn[1], mine, mine, left)
    push(share[0], mine, mine, sibling)
    from_left = outs.at[k, :, qcols((x + 3) % 4)]
    from_right = outs.at[k, :, qcols((x + 1) % 4)]
    got(turn[0], from_left)
    near = outs.at[k, :, qcols((x + 3) % 4, 0, half)]
    push(turn[2], near, near, right)
    push(share[1], from_left, from_left, sibling)
    got(turn[1], from_right)
    near = outs.at[k, :, qcols((x + 1) % 4, half, half)]
    push(turn[3], near, near, left)
    push(share[2], from_right, from_right, sibling)
    opposite = outs.at[k, :, qcols((x + 2) % 4)]
    got(turn[2], outs.at[k, :, qcols((x + 2) % 4, 0, half)])
    got(turn[3], outs.at[k, :, qcols((x + 2) % 4, half, half)])
    push(share[3], opposite, opposite, sibling)
    for n, q in enumerate((x, (x + 3) % 4, (x + 1) % 4, (x + 2) % 4)):
        got(share[n], outs.at[other, :, qcols(q)])
    final = pltpu.make_async_copy(outs, out_hbm, ls.at[6])
    final.start()
    for c in pending:
        c.wait_send()
    for g in range(2):
        for d in range(1, 4):
            zz = (z + d) % 4

            @pl.when(pair(zz))
            def _(g=g, d=d, zz=zz):
                copy(
                    tile_ids[g, d, 1], yy.at[g, :, tcols(head(zz) + 1)], zr.at[g, d - 1, 1],
                    sibling,
                ).wait_send()

    @pl.when(pair(z))
    def _():
        for d in range(1, 4):
            second = outs.at[k, :, tcols(head(z) + 1, base)]
            copy(last_ids[d, 1], second, second, sibling).wait_send()

    for c in grad_copies:
        c.wait()
    final.wait()


def slot_tables(routes, router_weight, order, capacity):
    hit_table = (routes[:, :, None] == order).astype(jnp.int32)
    per_token = jnp.sum(hit_table, axis=1)
    before = jnp.cumsum(per_token, axis=0) - per_token
    slot_of = jnp.sum(hit_table * before[:, None, :], axis=2)
    slot_ids = jnp.arange(capacity, dtype=jnp.int32)
    placed = hit_table[:, :, :, None] * (slot_of[:, :, None, None] == slot_ids).astype(jnp.int32)
    tok_rows = routes.shape[0]
    flat = placed.reshape(tok_rows, 2, order.shape[0] * capacity).astype(jnp.float32)
    slot_weight = jnp.sum(flat * router_weight[:, :, None], axis=(0, 1))
    return (flat[:, 0], flat[:, 1], slot_weight)


def on_device(tokens, cotangent, routes, router_weight, w_gate, w_up, w_down):
    experts = lax.axis_size("dp")
    dims = Dims(tokens.shape[0], tokens.shape[1], w_gate.shape[2])
    cap, grp = dims.cap, dims.grp
    core = lax.axis_index("fsdp") % 2
    order = jnp.arange(experts, dtype=jnp.int32).reshape(NY, NZH).T.reshape(-1)
    first_pick, second_pick, slot_weight = slot_tables(routes, router_weight, order, cap)
    picked = (first_pick + second_pick).astype(BF)
    mine = jnp.where(core == 0, tokens, cotangent)
    scale = jnp.where(core == 0, 1.0, slot_weight)
    rows = lax.dot_general(picked, mine, LEAD, preferred_element_type=F32)
    send = (rows * scale[:, None]).astype(BF).reshape(2, grp, dims.feat)
    pick_w = jnp.where(core == 0, router_weight, 1.0)
    vmem = pl.BlockSpec(memory_space=pltpu.VMEM)
    hbm = pl.BlockSpec(memory_space=pl.ANY)
    feat, hid, half, quart, tile = dims.feat, dims.hid, dims.half, dims.quart, dims.tile
    outs, gg, gu, gd = pl.pallas_call(
        functools.partial(experts_kernel, dims),
        out_shape=(
            jax.ShapeDtypeStruct((2, dims.tok, feat), BF),
            jax.ShapeDtypeStruct((feat, hid), BF),
            jax.ShapeDtypeStruct((feat, hid), BF),
            jax.ShapeDtypeStruct((hid, feat), BF),
        ),
        in_specs=[vmem] * 4 + [hbm] * 3,
        out_specs=(hbm,) * 4,
        scratch_shapes=[
            pltpu.VMEM((2, 2, grp, feat), BF),
            pltpu.VMEM((feat, hid), BF),
            pltpu.VMEM((feat, hid), BF),
            pltpu.VMEM((hid, feat), BF),
            pltpu.VMEM((2, grp, hid), BF),
            pltpu.VMEM((2, grp, hid), BF),
            pltpu.VMEM((2, grp, hid), BF),
            pltpu.VMEM((2, 2, grp, feat), BF),
            pltpu.VMEM((2, grp, feat), BF),
            pltpu.VMEM((2, grp, half), BF),
            pltpu.VMEM((2, grp, half), BF),
            pltpu.VMEM((2, grp, quart), BF),
            pltpu.VMEM((2, grp, quart), BF),
            pltpu.VMEM((2, grp, quart), BF),
            pltpu.VMEM((2, 3, 2, grp, tile), BF),
            pltpu.VMEM((2, grp, 2 * tile), BF),
            pltpu.VMEM((2, grp, 2 * tile), BF),
            pltpu.VMEM((2, dims.tok, feat), BF),
            pltpu.VMEM((feat, hid), BF),
            pltpu.VMEM((feat, hid), BF),
            pltpu.VMEM((hid, feat), BF),
            pltpu.SemaphoreType.DMA((96,)),
            pltpu.SemaphoreType.DMA((96,)),
            pltpu.SemaphoreType.DMA((7,)),
        ],
        compiler_params=pltpu.CompilerParams(
            collective_id=0, has_side_effects=True, vmem_limit_bytes=60 * 1024 * 1024
        ),
        name="experts",
    )(send, first_pick.astype(BF), second_pick.astype(BF), pick_w, w_gate[0], w_up[0], w_down[0])
    return (outs[0], outs[1], gg[None], gu[None], gd[None])


def solution(mesh):
    return jax.shard_map(
        on_device,
        mesh=mesh,
        in_specs=(
            P("dp", None),
            P("dp", None),
            P("dp", None),
            P("dp", None),
            P("dp", None, "fsdp"),
            P("dp", None, "fsdp"),
            P("dp", "fsdp", None),
        ),
        out_specs=(
            P("dp", None),
            P("dp", None),
            P("dp", None, "fsdp"),
            P("dp", None, "fsdp"),
            P("dp", "fsdp", None),
        ),
        check_vma=False,
    )
```

```python
import functools

import jax
import jax.numpy as jnp
from jax import lax
from jax.experimental import pallas as pl
from jax.experimental.pallas import tpu as pltpu
from jax.sharding import PartitionSpec as P

MESH = pl.DeviceIdType.MESH
NY, NZH, NZ, NX, NC = 4, 2, 4, 4, 2
BF, F32 = jnp.bfloat16, jnp.float32
TRAIL = (((1,), (1,)), ((), ()))
LEAD = (((0,), (0,)), ((), ()))


class Dims:
    def __init__(self, tok, feat, hid):
        self.tok, self.feat, self.hid = tok, feat, hid
        self.cap = tok * 3 // 8
        self.grp = NY * self.cap
        self.quart = feat // NX
        self.half = self.quart // 2
        self.tile = self.quart // 6


def experts_kernel(
    dims,
    routes, weights, tokens_hbm, cotangent_hbm, gate_hbm, up_hbm, down_hbm,
    out_hbm, dx_hbm, sx_hbm, sdy_hbm, hid_hbm, gdy_hbm, udy_hbm,
    mine, first, second, send,
    arr, wg, wu, wd, hid, gdy, udy, tt, dd, rl1, rr1, rl2, rr2, yy, zr, ww, uu, outs,
    ss, rs, ls,
):
    scope = jax.named_scope
    cap, grp, quart, half, tile = dims.cap, dims.grp, dims.quart, dims.half, dims.tile
    dp, fs = lax.axis_index("dp"), lax.axis_index("fsdp")
    y, zh = dp // 2, dp % 2
    z, x, k = fs // 8, (fs // 2) % 4, fs % 2
    other = 1 - k

    def dev(yy_, zh_, z_, x_, k_):
        return (yy_ * 2 + zh_, (z_ * 4 + x_) * 2 + k_)

    def up_y(d):
        return (y + d) % 4

    right, left = dev(y, zh, z, (x + 1) % 4, k), dev(y, zh, z, (x + 3) % 4, k)
    sibling = dev(y, zh, z, x, other)

    used = [0]
    pending = []

    def fresh():
        used[0] += 1
        return used[0] - 1

    def copy(i, src, dst, to):
        return pltpu.make_async_remote_copy(
            src_ref=src, dst_ref=dst, send_sem=ss.at[i], recv_sem=rs.at[i],
            device_id=to, device_id_type=MESH,
        )

    def push(i, src, dst, to):
        c = copy(i, src, dst, to)
        c.start()
        pending.append(c)

    def got(i, region):
        copy(i, region, region, sibling).wait_recv()

    def qcols(q, off=0, width=None):
        return pl.ds(pl.multiple_of(q * quart + off, 128), quart if width is None else width)

    def rows_of(b):
        return pl.ds(pl.multiple_of(b * cap, 16), cap)

    def tcols(t, base=0):
        return pl.ds(pl.multiple_of(base + t * tile, 128), tile)

    barrier = pltpu.get_barrier_semaphore()
    partners = [right, left, sibling]
    for d in range(1, 4):
        partners.append(dev(y, zh, (z + d) % 4, x, k))
    for d in range(4):
        if d:
            partners.append(dev(up_y(d), zh, z, x, k))
        partners.append(dev(up_y(d), 1 - zh, z, x, k))
    for p in partners:
        pl.semaphore_signal(barrier, inc=1, device_id=p, device_id_type=MESH)

    @pl.when(k == 0)
    def _():
        pltpu.make_async_copy(tokens_hbm, mine, ls.at[3]).start()

    @pl.when(k == 1)
    def _():
        pltpu.make_async_copy(cotangent_hbm, mine, ls.at[3]).start()

    loads = [
        pltpu.make_async_copy(s, d, ls.at[n])
        for n, (s, d) in enumerate(((gate_hbm, wg), (up_hbm, wu), (down_hbm, wd)))
    ]
    for c in loads:
        c.start()

    experts = NY * NZH
    seat = lax.broadcasted_iota(jnp.int32, (experts, dims.tok), 0)
    expert = (seat % NY) * NZH + seat // NY
    hit_first = (routes[0:1, :] == expert).astype(F32)
    hit_second = (routes[1:2, :] == expert).astype(F32)
    earlier = (
        lax.broadcasted_iota(jnp.int32, (dims.tok, dims.tok), 0)
        < lax.broadcasted_iota(jnp.int32, (dims.tok, dims.tok), 1)
    ).astype(F32).astype(BF)
    place = jnp.dot(
        (hit_first + hit_second).astype(BF), earlier, preferred_element_type=F32
    )
    slot = lax.broadcasted_iota(jnp.int32, (cap, dims.tok), 0).astype(F32)
    for e in range(experts):
        here = (place[e : e + 1, :] == slot).astype(F32)
        at = pl.ds((e % NY) * cap, cap)
        first[e // NY, at] = (here * hit_first[e : e + 1, :]).astype(BF)
        second[e // NY, at] = (here * hit_second[e : e + 1, :]).astype(BF)

    def fill(g, at):
        f, s = first[g].astype(F32), second[g].astype(F32)
        scale = jnp.sum(f * weights[0:1, :] + s * weights[1:2, :], axis=1, keepdims=True)
        scale = jnp.where(k == 0, jnp.ones_like(scale), scale)
        send[g, :, at] = (
            jnp.dot((f + s).astype(BF), mine[:, at], preferred_element_type=F32) * scale
        ).astype(BF)

    zc = 1 - zh
    pltpu.make_async_copy(tokens_hbm, mine, ls.at[3]).wait()
    with scope("fill_cross"):
        fill(zc, qcols(x))
    with scope("barrier"):
        pl.semaphore_wait(barrier, len(partners))
    ring_order = [(0, 2), (1, 0), (1, 1), (1, 3), (1, 2)]
    send_ids = {(g, d): fresh() for g in range(2) for d in range(4)}
    both_ids = {(g, d): fresh() for g in range(2) for d in range(4)}
    ring = {b: [fresh() for _ in range(4)] for b in ring_order}
    for d in (0, 1, 3, 2):
        push(
            send_ids[1, d],
            send.at[zc, rows_of(up_y(d)), qcols(x)],
            arr.at[k, zh, rows_of(y), qcols(x)],
            dev(up_y(d), zc, z, x, k),
        )
    with scope("fill_same"):
        for q in (x, (x + 1) % 4, (x + 2) % 4, (x + 3) % 4):
            fill(zh, qcols(q))
    push(
        send_ids[0, 2],
        send.at[zh, rows_of(up_y(2)), qcols(x)],
        arr.at[k, zh, rows_of(y), qcols(x)],
        dev(up_y(2), zh, z, x, k),
    )
    for d in (1, 3):
        push(
            send_ids[0, d],
            send.at[zh, rows_of(up_y(d))],
            arr.at[k, zh, rows_of(y)],
            dev(up_y(d), zh, z, x, k),
        )
    push(both_ids[0, 0], send.at[zh, rows_of(y)], arr.at[k, zh, rows_of(y)], sibling)
    arr[k, zh, rows_of(y)] = send[zh, rows_of(y)]

    def block_of(b, *cols):
        g, d = b
        rows = rows_of(up_y(4 - d) if d else y)
        return arr.at[(k, zc if g else zh, rows) + cols]

    def ring_one(b):
        with scope(f"ring_one_{b[0]}{b[1]}"):
            near = block_of(b, qcols(x))
            got(send_ids[b], near)
            push(ring[b][0], near, near, right)
            push(ring[b][1], near, near, left)

    def ring_two(b):
        with scope(f"ring_two_{b[0]}{b[1]}"):
            got(ring[b][0], block_of(b, qcols((x + 3) % 4)))
            near = block_of(b, qcols((x + 3) % 4, 0, half))
            push(ring[b][2], near, near, right)
            got(ring[b][1], block_of(b, qcols((x + 1) % 4)))
            near = block_of(b, qcols((x + 1) % 4, half, half))
            push(ring[b][3], near, near, left)

    def ring_end(b):
        with scope(f"ring_end_{b[0]}{b[1]}"):
            got(ring[b][2], block_of(b, qcols((x + 2) % 4, 0, half)))
            got(ring[b][3], block_of(b, qcols((x + 2) % 4, half, half)))
            push(both_ids[b], block_of(b), block_of(b), sibling)

    def same_block(d):
        with scope(f"same_block_{d}"):
            got(send_ids[0, d], block_of((0, d)))
            push(both_ids[0, d], block_of((0, d)), block_of((0, d)), sibling)

    def both_here(g):
        with scope(f"both_here_{g}"):
            for d in range(4):
                rows = rows_of(up_y(4 - d) if d else y)
                got(both_ids[g, d], arr.at[other, zc if g else zh, rows])

    def first_stage(g):
        zg = zh if g == 0 else zc
        gate_pre = jnp.dot(arr[0, zg], wg[...], preferred_element_type=F32)
        up_pre = jnp.dot(arr[0, zg], wu[...], preferred_element_type=F32)
        hidden_dy = lax.dot_general(arr[1, zg], wd[...], TRAIL, preferred_element_type=F32)
        sigma = jax.nn.sigmoid(gate_pre)
        active = gate_pre * sigma
        hid[zg] = (active * up_pre).astype(BF)
        gdy[zg] = (hidden_dy * up_pre * sigma * (1.0 + gate_pre * (1.0 - sigma))).astype(BF)
        udy[zg] = (hidden_dy * active).astype(BF)

    quarters = [(x + 2) % 4, (x + 1) % 4, (x + 3) % 4, x]
    swap_ids = {(g, n): fresh() for g in range(2) for n in range(4)}

    hop_ids = {(g, n): fresh() for g in range(2) for n in range(6)}

    def plus(a, b):
        return (a.astype(F32) + b.astype(F32)).astype(BF)

    def chip_sum(g, n):
        q = quarters[n]
        got(swap_ids[g, n], dd.at[g, :, qcols(q)])
        tt[g, k, :, qcols(q)] = plus(tt[g, k, :, qcols(q)], dd[g, :, qcols(q)])
        if n == 0:
            push(hop_ids[g, 0], tt.at[g, k, :, qcols(q, 0, half)], rl1.at[g], right)
            push(hop_ids[g, 1], tt.at[g, k, :, qcols(q, half, half)], rr1.at[g], left)
        if n == 1:
            push(
                hop_ids[g, 2], tt.at[g, k, :, qcols(q, half, half)],
                rl2.at[g, :, pl.ds(half, half)], right,
            )
        if n == 2:
            push(
                hop_ids[g, 3], tt.at[g, k, :, qcols(q, 0, half)],
                rr2.at[g, :, pl.ds(0, half)], left,
            )

    def second_stage(g):
        zg = zh if g == 0 else zc
        width = quart // 3
        for n, q in enumerate(quarters):

            def body(c, carry, q=q):
                at = pl.ds(pl.multiple_of(q * quart + c * width, 128), width)
                tt[g, 0, :, at] = jnp.dot(
                    hid[zg], wd[:, at], preferred_element_type=F32
                ).astype(BF)
                tt[g, 1, :, at] = (
                    lax.dot_general(gdy[zg], wg[at, :], TRAIL, preferred_element_type=F32)
                    + lax.dot_general(udy[zg], wu[at, :], TRAIL, preferred_element_type=F32)
                ).astype(BF)
                return carry

            with scope(f"second_{g}{n}"):
                lax.fori_loop(0, 3, body, 0)
            push(swap_ids[g, n], tt.at[g, other, :, qcols(q)], dd.at[g, :, qcols(q)], sibling)
            if n:
                with scope(f"chip_sum_{g}{n - 1}"):
                    chip_sum(g, n - 1)

    def hop_two(g):
        got(hop_ids[g, 0], rl1.at[g])
        at = qcols(quarters[1], 0, half)
        tt[g, k, :, at] = plus(tt[g, k, :, at], rl1[g])
        push(hop_ids[g, 4], tt.at[g, k, :, at], rl2.at[g, :, pl.ds(0, half)], right)
        got(hop_ids[g, 1], rr1.at[g])
        at = qcols(quarters[2], half, half)
        tt[g, k, :, at] = plus(tt[g, k, :, at], rr1[g])
        push(hop_ids[g, 5], tt.at[g, k, :, at], rr2.at[g, :, pl.ds(half, half)], left)

    def head(zz):
        return (3 * zz + 1 - k) // 2

    def pair(zz):
        return (zz + k) % 2 == 0

    tile_ids = {(g, d, s): fresh() for g in range(2) for d in range(1, 4) for s in range(2)}

    def along_z(g):
        chip_sum(g, 3)
        for n in (2, 3, 4, 5):
            region = (rl2 if n in (2, 4) else rr2).at[
                g, :, pl.ds(half if n in (2, 5) else 0, half)
            ]
            got(hop_ids[g, n], region)
        yy[g] = (
            tt[g, k, :, qcols(x)].astype(F32) + rl2[g].astype(F32) + rr2[g].astype(F32)
        ).astype(BF)
        for d in range(1, 4):
            zz = (z + d) % 4
            to = dev(y, zh, zz, x, k)
            push(tile_ids[g, d, 0], yy.at[g, :, tcols(head(zz))], zr.at[g, d - 1, 0], to)

            @pl.when(pair(zz))
            def _(d=d, zz=zz, to=to):
                copy(
                    tile_ids[g, d, 1], yy.at[g, :, tcols(head(zz) + 1)], zr.at[g, d - 1, 1], to
                ).start()

    back_ids = {(g, d): fresh() for g in range(2) for d in range(4)}

    def home(g):
        zg = zh if g == 0 else zc

        def summed(s):
            total = yy[g, :, tcols(head(z) + s)].astype(F32)
            for d in range(1, 4):
                total = total + zr[g, d - 1, s].astype(F32)
            ww[g, :, pl.ds(s * tile, tile)] = total.astype(BF)

        for d in range(1, 4):
            got(tile_ids[g, d, 0], zr.at[g, d - 1, 0])
        summed(0)

        @pl.when(pair(z))
        def _():
            for d in range(1, 4):
                got(tile_ids[g, d, 1], zr.at[g, d - 1, 1])
            summed(1)

        @pl.when(jnp.logical_not(pair(z)))
        def _():
            ww[g, :, pl.ds(tile, tile)] = jnp.zeros((grp, tile), BF)

        for d in (1, 3, 2, 0):
            if g == 0 and d == 0:
                uu[zh, rows_of(y)] = ww[0, rows_of(y)]
            else:
                push(
                    back_ids[g, d], ww.at[g, rows_of(up_y(d))], uu.at[zh, rows_of(y)],
                    dev(up_y(d), zg, z, x, k),
                )

    for b in ring_order:
        ring_one(b)
    for d in (1, 3):
        same_block(d)
    for b in ring_order:
        ring_two(b)
    ring_end((0, 2))
    with scope("weights_here"):
        for c in loads:
            c.wait()
    both_here(0)
    with scope("first_0"):
        first_stage(0)
    for b in ring_order[1:]:
        ring_end(b)
    second_stage(0)
    both_here(1)
    stores = [
        pltpu.make_async_copy(s, d, ls.at[4 + n])
        for n, (s, d) in enumerate(((arr.at[0], sx_hbm), (arr.at[1], sdy_hbm)))
    ]
    with scope("first_1"):
        first_stage(1)
    stores += [
        pltpu.make_async_copy(s, d, ls.at[6 + n])
        for n, (s, d) in enumerate(((hid, hid_hbm), (gdy, gdy_hbm), (udy, udy_hbm)))
    ]
    for c in stores:
        c.start()
    with scope("hop_two_0"):
        hop_two(0)
    second_stage(1)
    with scope("along_z_0"):
        along_z(0)
    with scope("hop_two_1"):
        hop_two(1)
    with scope("home_0"):
        home(0)
    with scope("along_z_1"):
        along_z(1)
    with scope("home_1"):
        home(1)

    with scope("wait_home"):
        for g in range(2):
            zg = zh if g == 0 else zc
            for d in range(4):
                if g or d:
                    got(back_ids[g, d], uu.at[zg, rows_of(up_y(4 - d) if d else y)])
    slots = uu[...].reshape(2 * grp, 2 * tile)
    same_token = (
        lax.broadcasted_iota(jnp.int32, (dims.tok, dims.tok), 0)
        == lax.broadcasted_iota(jnp.int32, (dims.tok, dims.tok), 1)
    )
    share_first = jnp.sum(
        jnp.where(same_token, weights[0:1, :], 0.0), axis=1, keepdims=True
    )
    share_second = jnp.sum(
        jnp.where(same_token, weights[1:2, :], 0.0), axis=1, keepdims=True
    )
    share_first = jnp.where(k == 0, share_first, jnp.ones_like(share_first))
    share_second = jnp.where(k == 0, share_second, jnp.ones_like(share_second))
    mixed = (
        share_first
        * lax.dot_general(
            first[...].reshape(2 * grp, dims.tok), slots, LEAD, preferred_element_type=F32
        )
        + share_second
        * lax.dot_general(
            second[...].reshape(2 * grp, dims.tok), slots, LEAD, preferred_element_type=F32
        )
    ).astype(BF)
    base = x * quart
    outs[k, :, tcols(head(z), base)] = mixed[:, :tile]

    @pl.when(pair(z))
    def _():
        outs[k, :, tcols(head(z) + 1, base)] = mixed[:, tile:]

    last_ids = {(d, s): fresh() for d in range(1, 4) for s in range(2)}
    to_right = [fresh() for _ in range(6)][0]
    to_left = [fresh() for _ in range(6)][0]
    onward = [fresh() for _ in range(6)][0]
    swap_last = [fresh() for _ in range(4)]

    def cell(q, t):
        return outs.at[k, :, tcols(t, q * quart)]

    def each_tile(zz, action):
        action(0)
        pl.when(pair(zz))(lambda: action(1))

    def near_x(t):
        copy(to_right + t, cell(x, t), cell(x, t), right).start()
        copy(to_left + t, cell(x, t), cell(x, t), left).start()

    def first_out(s):
        t = head(z) + s
        near_x(t)
        for d in (1, 3, 2):
            to = dev(y, zh, (z + d) % 4, x, k)
            copy(last_ids[d, s], cell(x, t), cell(x, t), to).start()

    each_tile(z, first_out)
    with scope("last_z"):
        for d in (1, 3, 2):
            zz = (z + 4 - d) % 4

            def relay(s, d=d, zz=zz):
                t = head(zz) + s
                got(last_ids[d, s], cell(x, t))
                near_x(t)

            each_tile(zz, relay)
    push(swap_last[0], outs.at[k, :, qcols(x)], outs.at[k, :, qcols(x)], sibling)
    with scope("last_x"):
        for d in (0, 1, 3, 2):
            zz = (z + 4 - d) % 4

            def onwards(s, zz=zz):
                t = head(zz) + s
                from_left, from_right = cell((x + 3) % 4, t), cell((x + 1) % 4, t)
                got(to_right + t, from_left)

                @pl.when(t < 3)
                def _():
                    copy(onward + t, from_left, from_left, right).start()

                got(to_left + t, from_right)

                @pl.when(t >= 3)
                def _():
                    copy(onward + t, from_right, from_right, left).start()

            each_tile(zz, onwards)
    for n, q in ((1, (x + 3) % 4), (2, (x + 1) % 4)):
        push(swap_last[n], outs.at[k, :, qcols(q)], outs.at[k, :, qcols(q)], sibling)
    with scope("last_far"):
        for t in range(6):
            got(onward + t, cell((x + 2) % 4, t))
    far = outs.at[k, :, qcols((x + 2) % 4)]
    push(swap_last[3], far, far, sibling)
    with scope("last_swap"):
        for n, q in enumerate((x, (x + 3) % 4, (x + 1) % 4, (x + 2) % 4)):
            got(swap_last[n], outs.at[other, :, qcols(q)])
    results = [
        pltpu.make_async_copy(outs.at[n], d, ls.at[9 + n]) for n, d in enumerate((out_hbm, dx_hbm))
    ]
    for c in results:
        c.start()
    with scope("drain"):
        for c in pending:
            c.wait_send()
        for g in range(2):
            for d in range(1, 4):
                zz = (z + d) % 4

                @pl.when(pair(zz))
                def _(g=g, d=d, zz=zz):
                    copy(
                        tile_ids[g, d, 1], yy.at[g, :, tcols(head(zz) + 1)], zr.at[g, d - 1, 1],
                        sibling,
                    ).wait_send()

        def sent(s):
            mine_ = cell(x, head(z) + s)
            for d in range(1, 4):
                copy(last_ids[d, s], mine_, mine_, sibling).wait_send()

        each_tile(z, sent)
        for t in range(6):
            for i in (to_right, to_left, onward):
                copy(i + t, cell(x, t), cell(x, t), sibling).wait_send()
        for c in stores + results:
            c.wait()


def on_device(tokens, cotangent, routes, router_weight, w_gate, w_up, w_down):
    dims = Dims(tokens.shape[0], tokens.shape[1], w_gate.shape[2])
    grp, feat, hid = dims.grp, dims.feat, dims.hid
    half, quart, tile = dims.half, dims.quart, dims.tile
    vmem = pl.BlockSpec(memory_space=pltpu.VMEM)
    hbm = pl.BlockSpec(memory_space=pl.ANY)
    wide = jax.ShapeDtypeStruct((2, grp, feat), BF)
    narrow = jax.ShapeDtypeStruct((2, grp, hid), BF)
    whole = jax.ShapeDtypeStruct((dims.tok, feat), BF)
    output, input_grad, slot_x, slot_dy, hidden, gate_dy, up_dy = pl.pallas_call(
        functools.partial(experts_kernel, dims),
        out_shape=(whole, whole, wide, wide, narrow, narrow, narrow),
        in_specs=[vmem] * 2 + [hbm] * 5,
        out_specs=(hbm,) * 7,
        scratch_shapes=[
            pltpu.VMEM((dims.tok, feat), BF),
            pltpu.VMEM((2, grp, dims.tok), BF),
            pltpu.VMEM((2, grp, dims.tok), BF),
            pltpu.VMEM((2, grp, feat), BF),
            pltpu.VMEM((2, 2, grp, feat), BF),
            pltpu.VMEM((feat, hid), BF),
            pltpu.VMEM((feat, hid), BF),
            pltpu.VMEM((hid, feat), BF),
            pltpu.VMEM((2, grp, hid), BF),
            pltpu.VMEM((2, grp, hid), BF),
            pltpu.VMEM((2, grp, hid), BF),
            pltpu.VMEM((2, 2, grp, feat), BF),
            pltpu.VMEM((2, grp, feat), BF),
            pltpu.VMEM((2, grp, half), BF),
            pltpu.VMEM((2, grp, half), BF),
            pltpu.VMEM((2, grp, quart), BF),
            pltpu.VMEM((2, grp, quart), BF),
            pltpu.VMEM((2, grp, quart), BF),
            pltpu.VMEM((2, 3, 2, grp, tile), BF),
            pltpu.VMEM((2, grp, 2 * tile), BF),
            pltpu.VMEM((2, grp, 2 * tile), BF),
            pltpu.VMEM((2, dims.tok, feat), BF),
            pltpu.SemaphoreType.DMA((128,)),
            pltpu.SemaphoreType.DMA((128,)),
            pltpu.SemaphoreType.DMA((11,)),
        ],
        compiler_params=pltpu.CompilerParams(
            collective_id=0, has_side_effects=True, vmem_limit_bytes=56 * 1024 * 1024
        ),
        name="experts",
    )(routes.T, router_weight.T, tokens, cotangent, w_gate[0], w_up[0], w_down[0])
    rows = 2 * grp
    slot_x, slot_dy = slot_x.reshape(rows, feat), slot_dy.reshape(rows, feat)
    hidden, gate_dy, up_dy = (a.reshape(rows, hid) for a in (hidden, gate_dy, up_dy))

    def grad(left_rows, right_rows):
        return lax.dot_general(
            left_rows, right_rows, LEAD, preferred_element_type=F32
        ).astype(BF)[None]

    return (
        output, input_grad, grad(slot_x, gate_dy), grad(slot_x, up_dy), grad(hidden, slot_dy)
    )


def solution(mesh):
    return jax.shard_map(
        on_device,
        mesh=mesh,
        in_specs=(
            P("dp", None),
            P("dp", None),
            P("dp", None),
            P("dp", None),
            P("dp", None, "fsdp"),
            P("dp", None, "fsdp"),
            P("dp", "fsdp", None),
        ),
        out_specs=(
            P("dp", None),
            P("dp", None),
            P("dp", None, "fsdp"),
            P("dp", None, "fsdp"),
            P("dp", "fsdp", None),
        ),
        check_vma=False,
    )
```

```python
import functools

import jax
import jax.numpy as jnp
from jax import lax
from jax.experimental import pallas as pl
from jax.experimental.pallas import tpu as pltpu
from jax.sharding import PartitionSpec as P

MESH = pl.DeviceIdType.MESH
NY, NZH, NZ, NX, NC = 4, 2, 4, 4, 2
BF, F32 = jnp.bfloat16, jnp.float32
TRAIL = (((1,), (1,)), ((), ()))
LEAD = (((0,), (0,)), ((), ()))


class Dims:
    def __init__(self, tok, feat, hid):
        self.tok, self.feat, self.hid = tok, feat, hid
        self.cap = tok * 3 // 8
        self.grp = NY * self.cap
        self.quart = feat // NX
        self.half = self.quart // 2
        self.tile = self.quart // 6


def experts_kernel(
    dims,
    routes, weights, tokens_hbm, cotangent_hbm, gate_hbm, up_hbm, down_hbm,
    outs, gg, gu, gd,
    mine, first, second, send,
    arr, wg, wu, wd, hid, gdy, udy, tt, dd, rl1, rr1, rl2, rr2, yy, uu,
    ss, rs, ls,
):
    scope = jax.named_scope
    cap, grp, quart, half, tile = dims.cap, dims.grp, dims.quart, dims.half, dims.tile
    dp, fs = lax.axis_index("dp"), lax.axis_index("fsdp")
    y, zh = dp // 2, dp % 2
    z, x, k = fs // 8, (fs // 2) % 4, fs % 2
    other = 1 - k

    def dev(yy_, zh_, z_, x_, k_):
        return (yy_ * 2 + zh_, (z_ * 4 + x_) * 2 + k_)

    def up_y(d):
        return (y + d) % 4

    right, left = dev(y, zh, z, (x + 1) % 4, k), dev(y, zh, z, (x + 3) % 4, k)
    sibling = dev(y, zh, z, x, other)

    used = [0]
    pending = []

    def fresh():
        used[0] += 1
        return used[0] - 1

    def copy(i, src, dst, to):
        return pltpu.make_async_remote_copy(
            src_ref=src, dst_ref=dst, send_sem=ss.at[i], recv_sem=rs.at[i],
            device_id=to, device_id_type=MESH,
        )

    def push(i, src, dst, to):
        c = copy(i, src, dst, to)
        c.start()
        pending.append(c)

    def got(i, region):
        copy(i, region, region, sibling).wait_recv()

    def qcols(q, off=0, width=None):
        return pl.ds(pl.multiple_of(q * quart + off, 128), quart if width is None else width)

    def rows_of(b):
        return pl.ds(pl.multiple_of(b * cap, 16), cap)

    def tcols(t, base=0):
        return pl.ds(pl.multiple_of(base + t * tile, 128), tile)

    barrier = pltpu.get_barrier_semaphore()
    partners = [right, left, sibling]
    for d in range(4):
        for turn in range(4):
            if d or turn:
                partners.append(dev(up_y(d), zh, (z + turn) % 4, x, k))
            partners.append(dev(up_y(d), 1 - zh, (z + turn) % 4, x, k))
    for p in partners:
        pl.semaphore_signal(barrier, inc=1, device_id=p, device_id_type=MESH)

    @pl.when(k == 0)
    def _():
        pltpu.make_async_copy(tokens_hbm, mine, ls.at[3]).start()

    @pl.when(k == 1)
    def _():
        pltpu.make_async_copy(cotangent_hbm, mine, ls.at[3]).start()

    loads = [
        pltpu.make_async_copy(s, d, ls.at[n])
        for n, (s, d) in enumerate(((gate_hbm, wg), (up_hbm, wu), (down_hbm, wd)))
    ]
    for c in loads:
        c.start()

    experts = NY * NZH
    seat = lax.broadcasted_iota(jnp.int32, (experts, dims.tok), 0)
    expert = (seat % NY) * NZH + seat // NY
    hit_first = (routes[0:1, :] == expert).astype(F32)
    hit_second = (routes[1:2, :] == expert).astype(F32)
    earlier = (
        lax.broadcasted_iota(jnp.int32, (dims.tok, dims.tok), 0)
        < lax.broadcasted_iota(jnp.int32, (dims.tok, dims.tok), 1)
    ).astype(F32).astype(BF)
    place = jnp.dot(
        (hit_first + hit_second).astype(BF), earlier, preferred_element_type=F32
    )
    slot = lax.broadcasted_iota(jnp.int32, (cap, dims.tok), 0).astype(F32)
    for e in range(experts):
        here = (place[e : e + 1, :] == slot).astype(F32)
        at = pl.ds((e % NY) * cap, cap)
        first[e // NY, at] = (here * hit_first[e : e + 1, :]).astype(BF)
        second[e // NY, at] = (here * hit_second[e : e + 1, :]).astype(BF)

    def fill(g, at):
        f, s = first[g].astype(F32), second[g].astype(F32)
        scale = jnp.sum(f * weights[0:1, :] + s * weights[1:2, :], axis=1, keepdims=True)
        scale = jnp.where(k == 0, jnp.ones_like(scale), scale)
        send[g, :, at] = (
            jnp.dot((f + s).astype(BF), mine[:, at], preferred_element_type=F32) * scale
        ).astype(BF)

    zc = 1 - zh
    pltpu.make_async_copy(tokens_hbm, mine, ls.at[3]).wait()
    with scope("fill_cross"):
        fill(zc, qcols(x))
    with scope("barrier"):
        pl.semaphore_wait(barrier, len(partners))
    ring_order = [(0, 2), (1, 0), (1, 1), (1, 3), (1, 2)]
    send_ids = {(g, d): fresh() for g in range(2) for d in range(4)}
    both_ids = {(g, d): fresh() for g in range(2) for d in range(4)}
    ring = {b: [fresh() for _ in range(4)] for b in ring_order}
    for d in (0, 1, 3, 2):
        push(
            send_ids[1, d],
            send.at[zc, rows_of(up_y(d)), qcols(x)],
            arr.at[k, zh, rows_of(y), qcols(x)],
            dev(up_y(d), zc, z, x, k),
        )
    with scope("fill_same"):
        for q in (x, (x + 1) % 4, (x + 2) % 4, (x + 3) % 4):
            fill(zh, qcols(q))
    push(
        send_ids[0, 2],
        send.at[zh, rows_of(up_y(2)), qcols(x)],
        arr.at[k, zh, rows_of(y), qcols(x)],
        dev(up_y(2), zh, z, x, k),
    )
    for d in (1, 3):
        push(
            send_ids[0, d],
            send.at[zh, rows_of(up_y(d))],
            arr.at[k, zh, rows_of(y)],
            dev(up_y(d), zh, z, x, k),
        )
    push(both_ids[0, 0], send.at[zh, rows_of(y)], arr.at[k, zh, rows_of(y)], sibling)
    arr[k, zh, rows_of(y)] = send[zh, rows_of(y)]

    def block_of(b, *cols):
        g, d = b
        rows = rows_of(up_y(4 - d) if d else y)
        return arr.at[(k, zc if g else zh, rows) + cols]

    def ring_one(b):
        with scope(f"ring_one_{b[0]}{b[1]}"):
            near = block_of(b, qcols(x))
            got(send_ids[b], near)
            push(ring[b][0], near, near, right)
            push(ring[b][1], near, near, left)

    def ring_two(b):
        with scope(f"ring_two_{b[0]}{b[1]}"):
            got(ring[b][0], block_of(b, qcols((x + 3) % 4)))
            near = block_of(b, qcols((x + 3) % 4, 0, half))
            push(ring[b][2], near, near, right)
            got(ring[b][1], block_of(b, qcols((x + 1) % 4)))
            near = block_of(b, qcols((x + 1) % 4, half, half))
            push(ring[b][3], near, near, left)

    def ring_end(b):
        with scope(f"ring_end_{b[0]}{b[1]}"):
            got(ring[b][2], block_of(b, qcols((x + 2) % 4, 0, half)))
            got(ring[b][3], block_of(b, qcols((x + 2) % 4, half, half)))
            push(both_ids[b], block_of(b), block_of(b), sibling)

    def same_block(d):
        with scope(f"same_block_{d}"):
            got(send_ids[0, d], block_of((0, d)))
            push(both_ids[0, d], block_of((0, d)), block_of((0, d)), sibling)

    def both_here(g):
        with scope(f"both_here_{g}"):
            for d in range(4):
                rows = rows_of(up_y(4 - d) if d else y)
                got(both_ids[g, d], arr.at[other, zc if g else zh, rows])

    def first_stage(g):
        zg = zh if g == 0 else zc
        gate_pre = jnp.dot(arr[0, zg], wg[...], preferred_element_type=F32)
        up_pre = jnp.dot(arr[0, zg], wu[...], preferred_element_type=F32)
        hidden_dy = lax.dot_general(arr[1, zg], wd[...], TRAIL, preferred_element_type=F32)
        sigma = jax.nn.sigmoid(gate_pre)
        active = gate_pre * sigma
        hid[zg] = (active * up_pre).astype(BF)
        gdy[zg] = (hidden_dy * up_pre * sigma * (1.0 + gate_pre * (1.0 - sigma))).astype(BF)
        udy[zg] = (hidden_dy * active).astype(BF)

    quarters = [(x + 2) % 4, (x + 1) % 4, (x + 3) % 4, x]
    swap_ids = {(g, n): fresh() for g in range(2) for n in range(4)}

    hop_ids = {(g, h, n): fresh() for g in range(2) for h in range(2) for n in range(6)}
    part = grp // 2

    def plus(a, b):
        return (a.astype(F32) + b.astype(F32)).astype(BF)

    def rows_h(h):
        return pl.ds(h * part, part)

    def hop(g, h, n):
        q = quarters[(0, 0, 1, 2, 1, 2)[n]]
        off = (0, half, half, 0, 0, half)[n]
        rows = rows_h(h)
        source = tt.at[g, k, rows, qcols(q, off, half)]
        if n < 2:
            target = (rl1, rr1)[n].at[g, rows]
        else:
            target = (rl2 if n % 2 == 0 else rr2).at[g, rows, pl.ds(off, half)]
        push(hop_ids[g, h, n], source, target, right if n % 2 == 0 else left)

    def chip_sum(g, n):
        with scope(f"chip_sum_{g}{n}"):
            q = quarters[n]
            got(swap_ids[g, n], dd.at[g, :, qcols(q)])
            tt[g, k, :, qcols(q)] = plus(tt[g, k, :, qcols(q)], dd[g, :, qcols(q)])
            if n == 0:
                for h in range(2):
                    hop(g, h, 0)
                    hop(g, h, 1)
            if n in (1, 2):
                hop(g, 0, n + 1)

    def second_part(g, n):
        zg = zh if g == 0 else zc
        width = quart // 3
        q = quarters[n]

        def body(c, carry):
            at = pl.ds(pl.multiple_of(q * quart + c * width, 128), width)
            tt[g, 0, :, at] = jnp.dot(
                hid[zg], wd[:, at], preferred_element_type=F32
            ).astype(BF)
            tt[g, 1, :, at] = (
                lax.dot_general(gdy[zg], wg[at, :], TRAIL, preferred_element_type=F32)
                + lax.dot_general(udy[zg], wu[at, :], TRAIL, preferred_element_type=F32)
            ).astype(BF)
            return carry

        with scope(f"second_{g}{n}"):
            lax.fori_loop(0, 3, body, 0)
        push(swap_ids[g, n], tt.at[g, other, :, qcols(q)], dd.at[g, :, qcols(q)], sibling)

    def hop_two(g, h):
        with scope(f"hop_two_{g}{h}"):
            rows = rows_h(h)
            got(hop_ids[g, h, 0], rl1.at[g, rows])
            at = qcols(quarters[1], 0, half)
            tt[g, k, rows, at] = plus(tt[g, k, rows, at], rl1[g, rows])
            hop(g, h, 4)
            got(hop_ids[g, h, 1], rr1.at[g, rows])
            at = qcols(quarters[2], half, half)
            tt[g, k, rows, at] = plus(tt[g, k, rows, at], rr1[g, rows])
            hop(g, h, 5)

    def head(zz):
        return (3 * zz + 1 - k) // 2

    def pair(zz):
        return (zz + k) % 2 == 0

    home_ids = {(g, d): [fresh() for _ in range(NY)][0] for g in range(2) for d in range(4)}

    def home_copy(g, d, b, wide):
        width = 2 * tile if wide else tile
        zz = (z + d) % 4
        return pltpu.make_async_remote_copy(
            src_ref=yy.at[g, rows_of(b), pl.ds(pl.multiple_of(head(zz) * tile, 128), width)],
            dst_ref=uu.at[zh, d, rows_of(y), pl.ds(0, width)],
            send_sem=ss.at[home_ids[g, d] + b], recv_sem=rs.at[home_ids[g, d] + y],
            device_id=dev(b, zh if g == 0 else zc, zz, x, k), device_id_type=MESH,
        )

    def by_width(zz, action):
        pl.when(pair(zz))(lambda: action(True))
        pl.when(jnp.logical_not(pair(zz)))(lambda: action(False))

    def each_home(g, b, action):
        for d in (1, 3, 2, 0):
            zz = (z + d) % 4
            if g == 0 and d == 0:
                pl.when(b != y)(
                    lambda d=d, zz=zz: by_width(zz, lambda wide: action(home_copy(g, d, b, wide)))
                )
            else:
                by_width(zz, lambda wide, d=d: action(home_copy(g, d, b, wide)))

    def finish(g, h):
        with scope(f"finish_{g}{h}"):
            rows = rows_h(h)
            for n in (2, 3, 4, 5):
                got(
                    hop_ids[g, h, n],
                    (rl2 if n % 2 == 0 else rr2).at[
                        g, rows, pl.ds((0, half, half, 0, 0, half)[n], half)
                    ],
                )
            yy[g, rows] = (
                tt[g, k, rows, qcols(x)].astype(F32)
                + rl2[g, rows].astype(F32)
                + rr2[g, rows].astype(F32)
            ).astype(BF)
            for b in (2 * h, 2 * h + 1):
                each_home(g, b, lambda c: c.start())
                if g == 0:

                    @pl.when(b == y)
                    def _(b=b):
                        def keep(wide):
                            for s in range(2 if wide else 1):
                                uu[zh, 0, rows_of(y), pl.ds(s * tile, tile)] = yy[
                                    0, rows_of(b), tcols(head(z) + s)
                                ]

                        by_width(z, keep)

    def wait_home():
        def arrived(wide):
            width = 2 * tile if wide else tile
            for g in range(2):
                for d in range(4):
                    for b in range(NY):
                        region = uu.at[zc if g else zh, d, rows_of(b), pl.ds(0, width)]
                        wait = pltpu.make_async_remote_copy(
                            src_ref=region, dst_ref=region, send_sem=ss.at[home_ids[g, d] + b],
                            recv_sem=rs.at[home_ids[g, d] + b], device_id=sibling,
                            device_id_type=MESH,
                        )
                        if g == 0 and d == 0:
                            pl.when(b != y)(wait.wait_recv)
                        else:
                            wait.wait_recv()

        by_width(z, arrived)

    def weight_grads(begin, end):
        width = 256
        rows = 2 * grp

        def body(c, carry):
            at = pl.ds(pl.multiple_of(c * width, 128), width)
            xs = arr[0, :, :, at].reshape(rows, width)
            ys = arr[1, :, :, at].reshape(rows, width)
            gg[at, :] = lax.dot_general(
                xs, gdy[...].reshape(rows, dims.hid), LEAD, preferred_element_type=F32
            ).astype(BF)
            gu[at, :] = lax.dot_general(
                xs, udy[...].reshape(rows, dims.hid), LEAD, preferred_element_type=F32
            ).astype(BF)
            gd[:, at] = lax.dot_general(
                hid[...].reshape(rows, dims.hid), ys, LEAD, preferred_element_type=F32
            ).astype(BF)
            return carry

        with scope(f"weight_grads_{begin}"):
            lax.fori_loop(begin, end, body, 0)

    ring_one((0, 2))
    ring_one((1, 0))
    ring_two((0, 2))
    ring_one((1, 1))
    ring_end((0, 2))
    same_block(1)
    same_block(3)
    ring_one((1, 3))
    ring_two((1, 0))
    ring_one((1, 2))
    ring_two((1, 1))
    with scope("weights_here"):
        for c in loads:
            c.wait()
    both_here(0)
    with scope("first_0"):
        first_stage(0)
    ring_end((1, 0))
    ring_two((1, 3))
    second_part(0, 0)
    ring_two((1, 2))
    ring_end((1, 1))
    second_part(0, 1)
    chip_sum(0, 0)
    ring_end((1, 3))
    second_part(0, 2)
    chip_sum(0, 1)
    second_part(0, 3)
    chip_sum(0, 2)
    ring_end((1, 2))
    hop_two(0, 0)
    hop(0, 1, 2)
    hop(0, 1, 3)
    both_here(1)
    with scope("first_1"):
        first_stage(1)
    hop_two(0, 1)
    second_part(1, 0)
    second_part(1, 1)
    chip_sum(1, 0)
    second_part(1, 2)
    chip_sum(1, 1)
    second_part(1, 3)
    chip_sum(1, 2)
    chip_sum(0, 3)
    chip_sum(1, 3)
    finish(0, 0)
    hop_two(1, 0)
    hop(1, 1, 2)
    hop(1, 1, 3)
    finish(0, 1)
    hop_two(1, 1)
    chunks = dims.feat // 256
    weight_grads(0, chunks // 3)
    finish(1, 0)
    finish(1, 1)
    weight_grads(chunks // 3, chunks)

    @pl.when(jnp.logical_not(pair(z)))
    def _():
        uu[:, :, :, pl.ds(tile, tile)] = jnp.zeros((2, 4, grp, tile), BF)

    with scope("wait_home"):
        wait_home()
    total = uu[:, 0].astype(F32)
    for d in range(1, 4):
        total = total + uu[:, d].astype(F32)
    slots = total.astype(BF).reshape(2 * grp, 2 * tile)
    same_token = (
        lax.broadcasted_iota(jnp.int32, (dims.tok, dims.tok), 0)
        == lax.broadcasted_iota(jnp.int32, (dims.tok, dims.tok), 1)
    )
    share_first = jnp.sum(
        jnp.where(same_token, weights[0:1, :], 0.0), axis=1, keepdims=True
    )
    share_second = jnp.sum(
        jnp.where(same_token, weights[1:2, :], 0.0), axis=1, keepdims=True
    )
    share_first = jnp.where(k == 0, share_first, jnp.ones_like(share_first))
    share_second = jnp.where(k == 0, share_second, jnp.ones_like(share_second))
    mixed = (
        share_first
        * lax.dot_general(
            first[...].reshape(2 * grp, dims.tok), slots, LEAD, preferred_element_type=F32
        )
        + share_second
        * lax.dot_general(
            second[...].reshape(2 * grp, dims.tok), slots, LEAD, preferred_element_type=F32
        )
    ).astype(BF)
    base = x * quart
    outs[k, :, tcols(head(z), base)] = mixed[:, :tile]

    @pl.when(pair(z))
    def _():
        outs[k, :, tcols(head(z) + 1, base)] = mixed[:, tile:]

    last_ids = {(d, s): fresh() for d in range(1, 4) for s in range(2)}
    to_right = [fresh() for _ in range(6)][0]
    to_left = [fresh() for _ in range(6)][0]
    onward = [fresh() for _ in range(6)][0]
    swap_last = [fresh() for _ in range(4)]

    def cell(q, t):
        return outs.at[k, :, tcols(t, q * quart)]

    def each_tile(zz, action):
        action(0)
        pl.when(pair(zz))(lambda: action(1))

    def near_x(t):
        copy(to_right + t, cell(x, t), cell(x, t), right).start()
        copy(to_left + t, cell(x, t), cell(x, t), left).start()

    def first_out(s):
        t = head(z) + s
        near_x(t)
        for d in (1, 3, 2):
            to = dev(y, zh, (z + d) % 4, x, k)
            copy(last_ids[d, s], cell(x, t), cell(x, t), to).start()

    each_tile(z, first_out)
    with scope("last_z"):
        for d in (1, 3, 2):
            zz = (z + 4 - d) % 4

            def relay(s, d=d, zz=zz):
                t = head(zz) + s
                got(last_ids[d, s], cell(x, t))
                near_x(t)

            each_tile(zz, relay)
    push(swap_last[0], outs.at[k, :, qcols(x)], outs.at[k, :, qcols(x)], sibling)
    with scope("last_x"):
        for d in (0, 1, 3, 2):
            zz = (z + 4 - d) % 4

            def onwards(s, zz=zz):
                t = head(zz) + s
                from_left, from_right = cell((x + 3) % 4, t), cell((x + 1) % 4, t)
                got(to_right + t, from_left)

                @pl.when(t < 3)
                def _():
                    copy(onward + t, from_left, from_left, right).start()

                got(to_left + t, from_right)

                @pl.when(t >= 3)
                def _():
                    copy(onward + t, from_right, from_right, left).start()

            each_tile(zz, onwards)
    for n, q in ((1, (x + 3) % 4), (2, (x + 1) % 4)):
        push(swap_last[n], outs.at[k, :, qcols(q)], outs.at[k, :, qcols(q)], sibling)
    with scope("last_far"):
        for t in range(6):
            got(onward + t, cell((x + 2) % 4, t))
    far = outs.at[k, :, qcols((x + 2) % 4)]
    push(swap_last[3], far, far, sibling)
    with scope("last_swap"):
        for n, q in enumerate((x, (x + 3) % 4, (x + 1) % 4, (x + 2) % 4)):
            got(swap_last[n], outs.at[other, :, qcols(q)])
    with scope("drain"):
        for c in pending:
            c.wait_send()
        for g in range(2):
            for b in range(NY):
                each_home(g, b, lambda c: c.wait_send())

        def sent(s):
            mine_ = cell(x, head(z) + s)
            for d in range(1, 4):
                copy(last_ids[d, s], mine_, mine_, sibling).wait_send()

        each_tile(z, sent)
        for t in range(6):
            for i in (to_right, to_left, onward):
                copy(i + t, cell(x, t), cell(x, t), sibling).wait_send()


def store_kernel(outs, gg, gu, gd, out, dx, gg_hbm, gu_hbm, gd_hbm, sems):
    pairs = ((outs.at[0], out), (outs.at[1], dx), (gg, gg_hbm), (gu, gu_hbm), (gd, gd_hbm))
    copies = [pltpu.make_async_copy(s, d, sems.at[n]) for n, (s, d) in enumerate(pairs)]
    for c in copies:
        c.start()
    for c in copies:
        c.wait()


def on_device(tokens, cotangent, routes, router_weight, w_gate, w_up, w_down):
    dims = Dims(tokens.shape[0], tokens.shape[1], w_gate.shape[2])
    grp, feat, hid = dims.grp, dims.feat, dims.hid
    half, quart, tile = dims.half, dims.quart, dims.tile
    vmem = pl.BlockSpec(memory_space=pltpu.VMEM)
    hbm = pl.BlockSpec(memory_space=pl.ANY)
    whole = jax.ShapeDtypeStruct((dims.tok, feat), BF)
    tall, flat = (feat, hid), (hid, feat)
    results = pl.pallas_call(
        functools.partial(experts_kernel, dims),
        out_shape=(
            pltpu.VMEM((2, dims.tok, feat), BF),
            pltpu.VMEM(tall, BF),
            pltpu.VMEM(tall, BF),
            pltpu.VMEM(flat, BF),
        ),
        in_specs=[vmem] * 2 + [hbm] * 5,
        out_specs=(vmem,) * 4,
        scratch_shapes=[
            pltpu.VMEM((dims.tok, feat), BF),
            pltpu.VMEM((2, grp, dims.tok), BF),
            pltpu.VMEM((2, grp, dims.tok), BF),
            pltpu.VMEM((2, grp, feat), BF),
            pltpu.VMEM((2, 2, grp, feat), BF),
            pltpu.VMEM((feat, hid), BF),
            pltpu.VMEM((feat, hid), BF),
            pltpu.VMEM((hid, feat), BF),
            pltpu.VMEM((2, grp, hid), BF),
            pltpu.VMEM((2, grp, hid), BF),
            pltpu.VMEM((2, grp, hid), BF),
            pltpu.VMEM((2, 2, grp, feat), BF),
            pltpu.VMEM((2, grp, feat), BF),
            pltpu.VMEM((2, grp, half), BF),
            pltpu.VMEM((2, grp, half), BF),
            pltpu.VMEM((2, grp, quart), BF),
            pltpu.VMEM((2, grp, quart), BF),
            pltpu.VMEM((2, grp, quart), BF),
            pltpu.VMEM((2, 4, grp, 2 * tile), BF),
            pltpu.SemaphoreType.DMA((160,)),
            pltpu.SemaphoreType.DMA((160,)),
            pltpu.SemaphoreType.DMA((4,)),
        ],
        compiler_params=pltpu.CompilerParams(
            collective_id=0, has_side_effects=True, vmem_limit_bytes=48 * 1024 * 1024
        ),
        name="experts",
    )(routes.T, router_weight.T, tokens, cotangent, w_gate[0], w_up[0], w_down[0])
    output, input_grad, grad_gate, grad_up, grad_down = pl.pallas_call(
        store_kernel,
        out_shape=(
            whole, whole, jax.ShapeDtypeStruct(tall, BF), jax.ShapeDtypeStruct(tall, BF),
            jax.ShapeDtypeStruct(flat, BF),
        ),
        in_specs=[vmem] * 4,
        out_specs=(hbm,) * 5,
        scratch_shapes=[pltpu.SemaphoreType.DMA((5,))],
        compiler_params=pltpu.CompilerParams(vmem_limit_bytes=16 * 1024 * 1024),
        name="store",
    )(*(pltpu.with_memory_space_constraint(r, pltpu.VMEM) for r in results))
    return (output, input_grad, grad_gate[None], grad_up[None], grad_down[None])


def solution(mesh):
    return jax.shard_map(
        on_device,
        mesh=mesh,
        in_specs=(
            P("dp", None),
            P("dp", None),
            P("dp", None),
            P("dp", None),
            P("dp", None, "fsdp"),
            P("dp", None, "fsdp"),
            P("dp", "fsdp", None),
        ),
        out_specs=(
            P("dp", None),
            P("dp", None),
            P("dp", None, "fsdp"),
            P("dp", None, "fsdp"),
            P("dp", "fsdp", None),
        ),
        check_vma=False,
    )
```

```python
import functools

import jax
import jax.numpy as jnp
from jax import lax
from jax.experimental import pallas as pl
from jax.experimental.pallas import tpu as pltpu
from jax.sharding import PartitionSpec as P

MESH = pl.DeviceIdType.MESH
NY, NZH, NZ, NX, NC = 4, 2, 4, 4, 2
BF, F32 = jnp.bfloat16, jnp.float32
TRAIL = (((1,), (1,)), ((), ()))
LEAD = (((0,), (0,)), ((), ()))


class Dims:
    def __init__(self, tok, feat, hid):
        self.tok, self.feat, self.hid = tok, feat, hid
        self.cap = tok * 3 // 8
        self.grp = NY * self.cap
        self.quart = feat // NX
        self.half = self.quart // 2
        self.tile = self.quart // 6


def experts_kernel(
    dims,
    routes_hbm, weights_hbm, tokens_hbm, cotangent_hbm, gate_hbm, up_hbm, down_hbm,
    outs, gg, gu, gd,
    routes, weights, mine, first, second, send,
    arr, wg, wu, wd, hid, gdy, udy, tt, dd, rl1, rr1, rl2, rr2, yy, zr, ww, uu,
    ss, rs, ls,
):
    scope = jax.named_scope
    cap, grp, quart, half, tile = dims.cap, dims.grp, dims.quart, dims.half, dims.tile
    dp, fs = lax.axis_index("dp"), lax.axis_index("fsdp")
    y, zh = dp // 2, dp % 2
    z, x, k = fs // 8, (fs // 2) % 4, fs % 2
    other = 1 - k

    def dev(yy_, zh_, z_, x_, k_):
        return (yy_ * 2 + zh_, (z_ * 4 + x_) * 2 + k_)

    def up_y(d):
        return (y + d) % 4

    right, left = dev(y, zh, z, (x + 1) % 4, k), dev(y, zh, z, (x + 3) % 4, k)
    sibling = dev(y, zh, z, x, other)

    used, out_used, drains = [0], [0], []

    def fresh():
        used[0] += 1
        return used[0] - 1

    def group(region=None):
        out_used[0] += 1
        if region is not None:
            drains.append((out_used[0] - 1, region))
        return out_used[0] - 1

    def copy(o, i, src, dst, to):
        return pltpu.make_async_remote_copy(
            src_ref=src, dst_ref=dst, send_sem=ss.at[o], recv_sem=rs.at[i],
            device_id=to, device_id_type=MESH,
        )

    def push(o, i, src, dst, to):
        copy(o, i, src, dst, to).start()

    def got(i, region):
        copy(0, i, region, region, sibling).wait_recv()

    def drained(o, region):
        copy(o, 0, region, region, sibling).wait_send()

    def qcols(q, off=0, width=None):
        return pl.ds(pl.multiple_of(q * quart + off, 128), quart if width is None else width)

    def rows_of(b):
        return pl.ds(pl.multiple_of(b * cap, 16), cap)

    def tcols(t, base=0):
        return pl.ds(pl.multiple_of(base + t * tile, 128), tile)

    barrier = pltpu.get_barrier_semaphore()
    partners = [right, left, sibling]
    for d in range(4):
        partners.append(dev(up_y(d), 1 - zh, z, x, k))
        for turn in range(4):
            if d or turn:
                partners.append(dev(up_y(d), zh, (z + turn) % 4, x, k))
    for p in partners:
        pl.semaphore_signal(barrier, inc=1, device_id=p, device_id_type=MESH)

    tables = [
        pltpu.make_async_copy(routes_hbm, routes, ls.at[4]),
        pltpu.make_async_copy(weights_hbm, weights, ls.at[5]),
    ]
    for c in tables:
        c.start()

    @pl.when(k == 0)
    def _():
        pltpu.make_async_copy(tokens_hbm, mine, ls.at[3]).start()

    @pl.when(k == 1)
    def _():
        pltpu.make_async_copy(cotangent_hbm, mine, ls.at[3]).start()

    loads = [
        pltpu.make_async_copy(s, d, ls.at[n])
        for n, (s, d) in enumerate(((gate_hbm, wg), (up_hbm, wu), (down_hbm, wd)))
    ]
    for c in loads:
        c.start()
    for c in tables:
        c.wait()

    experts = NY * NZH
    seat = lax.broadcasted_iota(jnp.int32, (experts, dims.tok), 0)
    expert = (seat % NY) * NZH + seat // NY
    hit_first = (routes[0:1, :] == expert).astype(F32)
    hit_second = (routes[1:2, :] == expert).astype(F32)
    earlier = (
        lax.broadcasted_iota(jnp.int32, (dims.tok, dims.tok), 0)
        < lax.broadcasted_iota(jnp.int32, (dims.tok, dims.tok), 1)
    ).astype(F32).astype(BF)
    place = jnp.dot(
        (hit_first + hit_second).astype(BF), earlier, preferred_element_type=F32
    )
    slot = lax.broadcasted_iota(jnp.int32, (cap, dims.tok), 0).astype(F32)
    for e in range(experts):
        here = (place[e : e + 1, :] == slot).astype(F32)
        at = pl.ds((e % NY) * cap, cap)
        first[e // NY, at] = (here * hit_first[e : e + 1, :]).astype(BF)
        second[e // NY, at] = (here * hit_second[e : e + 1, :]).astype(BF)

    def fill(g, at):
        f, s = first[g].astype(F32), second[g].astype(F32)
        scale = jnp.sum(f * weights[0:1, :] + s * weights[1:2, :], axis=1, keepdims=True)
        scale = jnp.where(k == 0, jnp.ones_like(scale), scale)
        send[g, :, at] = (
            jnp.dot((f + s).astype(BF), mine[:, at], preferred_element_type=F32) * scale
        ).astype(BF)

    zc = 1 - zh
    pltpu.make_async_copy(tokens_hbm, mine, ls.at[3]).wait()
    with scope("fill_cross"):
        fill(zc, qcols(x))
    with scope("barrier"):
        pl.semaphore_wait(barrier, len(partners))
    ring_order = [(0, 2), (1, 0), (1, 1), (1, 3), (1, 2)]
    send_ids = {b: fresh() for b in ring_order + [(0, 1), (0, 3)]}
    both_ids = [fresh() for _ in range(2)]
    ring = {b: [fresh() for _ in range(4)] for b in ring_order}
    rows5 = pl.ds(0, len(ring_order) * cap // 3)
    fives = arr.at[0, 0, rows5, pl.ds(0, 3 * quart)]
    fives_half = arr.at[0, 0, rows5, pl.ds(0, 3 * half)]
    pair_ids = {d: fresh() for d in range(4)}
    own_half, pair_half = (z % 2) * half, (1 - z % 2) * half
    partner = dev(y, zh, z + 1 - 2 * (z % 2), x, k)
    out_quart = group(send.at[0, pl.ds(0, cap), pl.ds(0, 3 * quart)])
    out_pair = group(arr.at[0, 0, pl.ds(0, cap), pl.ds(0, 2 * quart)])
    out_full = group(send.at[0, pl.ds(0, 2 * cap)])
    out_both = [group(arr.at[0, 0]) for _ in range(2)]
    out_ring = [group(r) for r in (fives, fives, fives_half, fives_half)]
    for d in (0, 1, 3, 2):
        push(
            out_quart, send_ids[1, d],
            send.at[zc, rows_of(up_y(d)), qcols(x, own_half, half)],
            arr.at[k, zh, rows_of(y), qcols(x, own_half, half)],
            dev(up_y(d), zc, z, x, k),
        )
    with scope("fill_same"):
        for q in (x, (x + 1) % 4, (x + 2) % 4, (x + 3) % 4):
            fill(zh, qcols(q))
    push(
        out_quart, send_ids[0, 2],
        send.at[zh, rows_of(up_y(2)), qcols(x)],
        arr.at[k, zh, rows_of(y), qcols(x)],
        dev(up_y(2), zh, z, x, k),
    )
    for d in (1, 3):
        push(
            out_full, send_ids[0, d],
            send.at[zh, rows_of(up_y(d))],
            arr.at[k, zh, rows_of(y)],
            dev(up_y(d), zh, z, x, k),
        )
    push(
        out_both[0], both_ids[0], send.at[zh, rows_of(y)], arr.at[k, zh, rows_of(y)], sibling
    )
    arr[k, zh, rows_of(y)] = send[zh, rows_of(y)]

    def block_of(b, *cols):
        g, d = b
        rows = rows_of(up_y(4 - d) if d else y)
        return arr.at[(k, zc if g else zh, rows) + cols]

    def crossed(d):
        with scope(f"crossed_{d}"):
            part_ = block_of((1, d), qcols(x, own_half, half))
            got(send_ids[1, d], part_)
            push(out_pair, pair_ids[d], part_, part_, partner)

    def ring_one(b):
        with scope(f"ring_one_{b[0]}{b[1]}"):
            near = block_of(b, qcols(x))
            if b[0]:
                got(pair_ids[b[1]], block_of(b, qcols(x, pair_half, half)))
            else:
                got(send_ids[b], near)
            push(out_ring[0], ring[b][0], near, near, right)
            push(out_ring[1], ring[b][1], near, near, left)

    def ring_two(b):
        with scope(f"ring_two_{b[0]}{b[1]}"):
            got(ring[b][0], block_of(b, qcols((x + 3) % 4)))
            near = block_of(b, qcols((x + 3) % 4, 0, half))
            push(out_ring[2], ring[b][2], near, near, right)
            got(ring[b][1], block_of(b, qcols((x + 1) % 4)))
            near = block_of(b, qcols((x + 1) % 4, half, half))
            push(out_ring[3], ring[b][3], near, near, left)

    def ring_end(b):
        with scope(f"ring_end_{b[0]}{b[1]}"):
            got(ring[b][2], block_of(b, qcols((x + 2) % 4, 0, half)))
            got(ring[b][3], block_of(b, qcols((x + 2) % 4, half, half)))
            push(out_both[b[0]], both_ids[b[0]], block_of(b), block_of(b), sibling)

    def same_block(d):
        with scope(f"same_block_{d}"):
            got(send_ids[0, d], block_of((0, d)))
            push(out_both[0], both_ids[0], block_of((0, d)), block_of((0, d)), sibling)

    def both_here(g):
        with scope(f"both_here_{g}"):
            got(both_ids[g], arr.at[other, zc if g else zh])

    def first_stage(g):
        zg = zh if g == 0 else zc
        gate_pre = jnp.dot(arr[0, zg], wg[...], preferred_element_type=F32)
        up_pre = jnp.dot(arr[0, zg], wu[...], preferred_element_type=F32)
        hidden_dy = lax.dot_general(arr[1, zg], wd[...], TRAIL, preferred_element_type=F32)
        sigma = jax.nn.sigmoid(gate_pre)
        active = gate_pre * sigma
        hid[zg] = (active * up_pre).astype(BF)
        gdy[zg] = (hidden_dy * up_pre * sigma * (1.0 + gate_pre * (1.0 - sigma))).astype(BF)
        udy[zg] = (hidden_dy * active).astype(BF)

    quarters = [(x + 2) % 4, (x + 1) % 4, (x + 3) % 4, x]
    swap_ids = {(g, n): fresh() for g in range(2) for n in range(4)}
    out_swap = [group(dd.at[g]) for g in range(2)]
    out_hop = {
        (g, n): group(tt.at[g, 0, :, pl.ds(0, 3 * half)]) for g in range(2) for n in range(2)
    }

    hop_ids = {(g, h, n): fresh() for g in range(2) for h in range(2) for n in range(6)}
    part = grp // 2

    def plus(a, b):
        return (a.astype(F32) + b.astype(F32)).astype(BF)

    def rows_h(h):
        return pl.ds(h * part, part)

    def hop(g, h, n):
        q = quarters[(0, 0, 1, 2, 1, 2)[n]]
        off = (0, half, half, 0, 0, half)[n]
        rows = rows_h(h)
        source = tt.at[g, k, rows, qcols(q, off, half)]
        if n < 2:
            target = (rl1, rr1)[n].at[g, rows]
        else:
            target = (rl2 if n % 2 == 0 else rr2).at[g, rows, pl.ds(off, half)]
        push(out_hop[g, n % 2], hop_ids[g, h, n], source, target, right if n % 2 == 0 else left)

    def chip_sum(g, n):
        with scope(f"chip_sum_{g}{n}"):
            q = quarters[n]
            got(swap_ids[g, n], dd.at[g, :, qcols(q)])
            tt[g, k, :, qcols(q)] = plus(tt[g, k, :, qcols(q)], dd[g, :, qcols(q)])
            if n == 0:
                for h in range(2):
                    hop(g, h, 0)
                    hop(g, h, 1)
            if n in (1, 2):
                hop(g, 0, n + 1)

    def second_part(g, n):
        zg = zh if g == 0 else zc
        width = quart // 3
        q = quarters[n]

        def body(c, carry):
            at = pl.ds(pl.multiple_of(q * quart + c * width, 128), width)
            tt[g, 0, :, at] = jnp.dot(
                hid[zg], wd[:, at], preferred_element_type=F32
            ).astype(BF)
            tt[g, 1, :, at] = (
                lax.dot_general(gdy[zg], wg[at, :], TRAIL, preferred_element_type=F32)
                + lax.dot_general(udy[zg], wu[at, :], TRAIL, preferred_element_type=F32)
            ).astype(BF)
            return carry

        with scope(f"second_{g}{n}"):
            lax.fori_loop(0, 3, body, 0)
        push(
            out_swap[g], swap_ids[g, n], tt.at[g, other, :, qcols(q)], dd.at[g, :, qcols(q)],
            sibling,
        )

    def hop_two(g, h):
        with scope(f"hop_two_{g}{h}"):
            rows = rows_h(h)
            got(hop_ids[g, h, 0], rl1.at[g, rows])
            at = qcols(quarters[1], 0, half)
            tt[g, k, rows, at] = plus(tt[g, k, rows, at], rl1[g, rows])
            hop(g, h, 4)
            got(hop_ids[g, h, 1], rr1.at[g, rows])
            at = qcols(quarters[2], half, half)
            tt[g, k, rows, at] = plus(tt[g, k, rows, at], rr1[g, rows])
            hop(g, h, 5)

    def head(zz):
        return (3 * zz + 1 - k) // 2

    def pair(zz):
        return (zz + k) % 2 == 0

    home_ids = [fresh() for _ in range(5)]
    along_ids = {(h, d): fresh() for h in range(2) for d in range(1, 4)}
    out_home = [group() for _ in range(5)]
    out_along = {d: group() for d in range(1, 4)}

    def home_copy(d, b, wide):
        width = 2 * tile if wide else tile
        zz = (z + d) % 4
        return pltpu.make_async_remote_copy(
            src_ref=yy.at[0, rows_of(b), pl.ds(pl.multiple_of(head(zz) * tile, 128), width)],
            dst_ref=uu.at[zh, d, rows_of(y), pl.ds(0, width)],
            send_sem=ss.at[out_home[d]], recv_sem=rs.at[home_ids[d]],
            device_id=dev(b, zh, zz, x, k), device_id_type=MESH,
        )

    def by_width(zz, action):
        pl.when(pair(zz))(lambda: action(True))
        pl.when(jnp.logical_not(pair(zz)))(lambda: action(False))

    def each_home(b):
        for d in (2, 1, 3, 0):
            zz = (z + d) % 4
            if d == 0:
                pl.when(b != y)(
                    lambda d=d, zz=zz: by_width(zz, lambda wide: home_copy(d, b, wide).start())
                )
            else:
                by_width(zz, lambda wide, d=d: home_copy(d, b, wide).start())

    def along(h):
        rows = rows_h(h)
        for d in (2, 1, 3):
            zz = (z + d) % 4

            def go(wide, d=d, zz=zz):
                width = 2 * tile if wide else tile
                push(
                    out_along[d], along_ids[h, d],
                    yy.at[1, rows, pl.ds(pl.multiple_of(head(zz) * tile, 128), width)],
                    zr.at[d - 1, rows, pl.ds(0, width)], dev(y, zh, zz, x, k),
                )

            by_width(zz, go)

    def collect(h):
        def add(wide):
            rows, width = rows_h(h), 2 * tile if wide else tile
            for d in range(1, 4):
                got(along_ids[h, d], zr.at[d - 1, rows, pl.ds(0, width)])
            for s in range(2 if wide else 1):
                at = pl.ds(s * tile, tile)
                total = yy[1, rows, tcols(head(z) + s)].astype(F32)
                for d in range(1, 4):
                    total = total + zr[d - 1, rows, at].astype(F32)
                ww[rows, at] = total.astype(BF)
            for b in (2 * h, 2 * h + 1):
                push(
                    out_home[4], home_ids[4], ww.at[rows_of(b), pl.ds(0, width)],
                    uu.at[zh, 0, rows_of(y), pl.ds(0, width)], dev(b, zc, z, x, k),
                )

        with scope(f"collect_{h}"):
            by_width(z, add)

    def finish(g, h):
        with scope(f"finish_{g}{h}"):
            rows = rows_h(h)
            for n in (2, 3, 4, 5):
                got(
                    hop_ids[g, h, n],
                    (rl2 if n % 2 == 0 else rr2).at[
                        g, rows, pl.ds((0, half, half, 0, 0, half)[n], half)
                    ],
                )
            yy[g, rows] = (
                tt[g, k, rows, qcols(x)].astype(F32)
                + rl2[g, rows].astype(F32)
                + rr2[g, rows].astype(F32)
            ).astype(BF)
            if g == 1:
                along(h)
                return
            for b in (2 * h, 2 * h + 1):
                each_home(b)

                @pl.when(b == y)
                def _(b=b):
                    def keep(wide):
                        for s in range(2 if wide else 1):
                            uu[zh, 0, rows_of(y), pl.ds(s * tile, tile)] = yy[
                                0, rows_of(b), tcols(head(z) + s)
                            ]

                    by_width(z, keep)

    def wait_home():
        def arrived(wide):
            width = 2 * tile if wide else tile
            for d in range(4):
                rows = grp if d else (NY - 1) * cap
                got(home_ids[d], uu.at[zh, d, pl.ds(0, rows), pl.ds(0, width)])
            got(home_ids[4], uu.at[zc, 0, :, pl.ds(0, width)])

        by_width(z, arrived)

    def weight_grads(begin, end):
        width = 256
        rows = 2 * grp

        def body(c, carry):
            at = pl.ds(pl.multiple_of(c * width, 128), width)
            xs = arr[0, :, :, at].reshape(rows, width)
            ys = arr[1, :, :, at].reshape(rows, width)
            gg[at, :] = lax.dot_general(
                xs, gdy[...].reshape(rows, dims.hid), LEAD, preferred_element_type=F32
            ).astype(BF)
            gu[at, :] = lax.dot_general(
                xs, udy[...].reshape(rows, dims.hid), LEAD, preferred_element_type=F32
            ).astype(BF)
            gd[:, at] = lax.dot_general(
                hid[...].reshape(rows, dims.hid), ys, LEAD, preferred_element_type=F32
            ).astype(BF)
            return carry

        with scope(f"weight_grads_{begin}"):
            lax.fori_loop(begin, end, body, 0)

    ring_one((0, 2))
    crossed(0)
    crossed(1)
    ring_two((0, 2))
    crossed(3)
    ring_one((1, 0))
    crossed(2)
    ring_one((1, 1))
    ring_end((0, 2))
    ring_two((1, 0))
    ring_one((1, 3))
    ring_one((1, 2))
    same_block(1)
    same_block(3)
    ring_two((1, 1))
    with scope("weights_here"):
        for c in loads:
            c.wait()
    both_here(0)
    with scope("first_0"):
        first_stage(0)
    ring_two((1, 3))
    ring_end((1, 0))
    second_part(0, 0)
    ring_two((1, 2))
    ring_end((1, 1))
    second_part(0, 1)
    chip_sum(0, 0)
    ring_end((1, 3))
    second_part(0, 2)
    chip_sum(0, 1)
    second_part(0, 3)
    chip_sum(0, 2)
    ring_end((1, 2))
    chip_sum(0, 3)
    hop_two(0, 0)
    hop(0, 1, 2)
    hop(0, 1, 3)
    both_here(1)
    with scope("first_1"):
        first_stage(1)
    second_part(1, 0)
    hop_two(0, 1)
    second_part(1, 1)
    chip_sum(1, 0)
    second_part(1, 2)
    chip_sum(1, 1)
    second_part(1, 3)
    chip_sum(1, 2)
    finish(0, 0)
    hop_two(1, 0)
    hop(1, 1, 2)
    hop(1, 1, 3)
    chip_sum(1, 3)
    finish(0, 1)
    hop_two(1, 1)
    chunks = dims.feat // 256
    weight_grads(0, chunks // 3)
    finish(1, 0)
    finish(1, 1)
    collect(0)
    collect(1)
    weight_grads(chunks // 3, chunks)

    @pl.when(jnp.logical_not(pair(z)))
    def _():
        uu[:, :, :, pl.ds(tile, tile)] = jnp.zeros((2, 4, grp, tile), BF)

    with scope("wait_home"):
        wait_home()
    total = uu[zh, 0].astype(F32)
    for d in range(1, 4):
        total = total + uu[zh, d].astype(F32)
    uu[zh, 0] = total.astype(BF)
    slots = uu[:, 0].reshape(2 * grp, 2 * tile)
    same_token = (
        lax.broadcasted_iota(jnp.int32, (dims.tok, dims.tok), 0)
        == lax.broadcasted_iota(jnp.int32, (dims.tok, dims.tok), 1)
    )
    share_first = jnp.sum(
        jnp.where(same_token, weights[0:1, :], 0.0), axis=1, keepdims=True
    )
    share_second = jnp.sum(
        jnp.where(same_token, weights[1:2, :], 0.0), axis=1, keepdims=True
    )
    share_first = jnp.where(k == 0, share_first, jnp.ones_like(share_first))
    share_second = jnp.where(k == 0, share_second, jnp.ones_like(share_second))
    mixed = (
        share_first
        * lax.dot_general(
            first[...].reshape(2 * grp, dims.tok), slots, LEAD, preferred_element_type=F32
        )
        + share_second
        * lax.dot_general(
            second[...].reshape(2 * grp, dims.tok), slots, LEAD, preferred_element_type=F32
        )
    ).astype(BF)
    base = x * quart
    outs[k, :, tcols(head(z), base)] = mixed[:, :tile]

    @pl.when(pair(z))
    def _():
        outs[k, :, tcols(head(z) + 1, base)] = mixed[:, tile:]

    last_ids = {(d, s): fresh() for d in range(1, 4) for s in range(2)}
    to_right = [fresh() for _ in range(6)][0]
    to_left = [fresh() for _ in range(6)][0]
    onward, swap_last = fresh(), fresh()
    out_last = [group(), group()]
    one_quart = outs.at[0, :, pl.ds(0, quart)]
    out_right, out_left, out_onward = (group(one_quart) for _ in range(3))
    out_swap_last = group(outs.at[0])

    def cell(q, t):
        return outs.at[k, :, tcols(t, q * quart)]

    def each_tile(zz, action):
        action(0)
        pl.when(pair(zz))(lambda: action(1))

    def near_x(t):
        push(out_right, to_right + t, cell(x, t), cell(x, t), right)
        push(out_left, to_left + t, cell(x, t), cell(x, t), left)

    def first_out(s):
        t = head(z) + s
        near_x(t)
        for d in (1, 3, 2):
            to = dev(y, zh, (z + d) % 4, x, k)
            push(out_last[s], last_ids[d, s], cell(x, t), cell(x, t), to)

    each_tile(z, first_out)
    with scope("last_z"):
        for d in (1, 3, 2):
            zz = (z + 4 - d) % 4

            def relay(s, d=d, zz=zz):
                t = head(zz) + s
                got(last_ids[d, s], cell(x, t))
                near_x(t)

            each_tile(zz, relay)
    def swap_quarter(q):
        cells = outs.at[k, :, qcols(q)]
        push(out_swap_last, swap_last, cells, cells, sibling)

    swap_quarter(x)
    with scope("last_x"):
        for d in (0, 1, 3, 2):
            zz = (z + 4 - d) % 4

            def onwards(s, zz=zz):
                t = head(zz) + s
                from_left, from_right = cell((x + 3) % 4, t), cell((x + 1) % 4, t)
                got(to_right + t, from_left)

                @pl.when(t < 3)
                def _():
                    push(out_onward, onward, from_left, from_left, right)

                got(to_left + t, from_right)

                @pl.when(t >= 3)
                def _():
                    push(out_onward, onward, from_right, from_right, left)

            each_tile(zz, onwards)
    swap_quarter((x + 3) % 4)
    swap_quarter((x + 1) % 4)
    with scope("last_far"):
        got(onward, outs.at[k, :, qcols((x + 2) % 4)])
    swap_quarter((x + 2) % 4)
    with scope("last_swap"):
        got(swap_last, outs.at[other])
    with scope("drain"):
        for o, region in drains:
            drained(o, region)
        for d in range(4):
            rows = grp if d else (NY - 1) * cap

            def sent_home(wide, d=d, rows=rows):
                width = 2 * tile if wide else tile
                drained(out_home[d], yy.at[0, pl.ds(0, rows), pl.ds(0, width)])
                if d:
                    drained(out_along[d], yy.at[1, :, pl.ds(0, width)])
                else:
                    drained(out_home[4], ww.at[:, pl.ds(0, width)])

            by_width((z + d) % 4, sent_home)
        each_tile(z, lambda s: drained(out_last[s], outs.at[0, :, pl.ds(0, 3 * tile)]))
    assert used[0] == rs.shape[0] and out_used[0] == ss.shape[0], (used, out_used)


def store_kernel(outs, gg, gu, gd, out, dx, gg_hbm, gu_hbm, gd_hbm, sems):
    pairs = ((outs.at[0], out), (outs.at[1], dx), (gg, gg_hbm), (gu, gu_hbm), (gd, gd_hbm))
    copies = [pltpu.make_async_copy(s, d, sems.at[n]) for n, (s, d) in enumerate(pairs)]
    for c in copies:
        c.start()
    for c in copies:
        c.wait()


def on_device(tokens, cotangent, routes, router_weight, w_gate, w_up, w_down):
    dims = Dims(tokens.shape[0], tokens.shape[1], w_gate.shape[2])
    grp, feat, hid = dims.grp, dims.feat, dims.hid
    half, quart, tile = dims.half, dims.quart, dims.tile
    vmem = pl.BlockSpec(memory_space=pltpu.VMEM)
    hbm = pl.BlockSpec(memory_space=pl.ANY)
    whole = jax.ShapeDtypeStruct((dims.tok, feat), BF)
    tall, flat = (feat, hid), (hid, feat)
    results = pl.pallas_call(
        functools.partial(experts_kernel, dims),
        out_shape=(
            pltpu.VMEM((2, dims.tok, feat), BF),
            pltpu.VMEM(tall, BF),
            pltpu.VMEM(tall, BF),
            pltpu.VMEM(flat, BF),
        ),
        in_specs=[hbm] * 7,
        out_specs=(vmem,) * 4,
        scratch_shapes=[
            pltpu.VMEM(routes.T.shape, jnp.int32),
            pltpu.VMEM(routes.T.shape, F32),
            pltpu.VMEM((dims.tok, feat), BF),
            pltpu.VMEM((2, grp, dims.tok), BF),
            pltpu.VMEM((2, grp, dims.tok), BF),
            pltpu.VMEM((2, grp, feat), BF),
            pltpu.VMEM((2, 2, grp, feat), BF),
            pltpu.VMEM((feat, hid), BF),
            pltpu.VMEM((feat, hid), BF),
            pltpu.VMEM((hid, feat), BF),
            pltpu.VMEM((2, grp, hid), BF),
            pltpu.VMEM((2, grp, hid), BF),
            pltpu.VMEM((2, grp, hid), BF),
            pltpu.VMEM((2, 2, grp, feat), BF),
            pltpu.VMEM((2, grp, feat), BF),
            pltpu.VMEM((2, grp, half), BF),
            pltpu.VMEM((2, grp, half), BF),
            pltpu.VMEM((2, grp, quart), BF),
            pltpu.VMEM((2, grp, quart), BF),
            pltpu.VMEM((2, grp, quart), BF),
            pltpu.VMEM((3, grp, 2 * tile), BF),
            pltpu.VMEM((grp, 2 * tile), BF),
            pltpu.VMEM((2, 4, grp, 2 * tile), BF),
            pltpu.SemaphoreType.DMA((29,)),
            pltpu.SemaphoreType.DMA((96,)),
            pltpu.SemaphoreType.DMA((6,)),
        ],
        compiler_params=pltpu.CompilerParams(
            collective_id=0, has_side_effects=True, vmem_limit_bytes=48 * 1024 * 1024
        ),
        name="experts",
    )(routes.T, router_weight.T, tokens, cotangent, w_gate[0], w_up[0], w_down[0])
    output, input_grad, grad_gate, grad_up, grad_down = pl.pallas_call(
        store_kernel,
        out_shape=(
            whole, whole, jax.ShapeDtypeStruct(tall, BF), jax.ShapeDtypeStruct(tall, BF),
            jax.ShapeDtypeStruct(flat, BF),
        ),
        in_specs=[vmem] * 4,
        out_specs=(hbm,) * 5,
        scratch_shapes=[pltpu.SemaphoreType.DMA((5,))],
        compiler_params=pltpu.CompilerParams(vmem_limit_bytes=16 * 1024 * 1024),
        name="store",
    )(*(pltpu.with_memory_space_constraint(r, pltpu.VMEM) for r in results))
    return (output, input_grad, grad_gate[None], grad_up[None], grad_down[None])


def solution(mesh):
    return jax.shard_map(
        on_device,
        mesh=mesh,
        in_specs=(
            P("dp", None),
            P("dp", None),
            P("dp", None),
            P("dp", None),
            P("dp", None, "fsdp"),
            P("dp", None, "fsdp"),
            P("dp", "fsdp", None),
        ),
        out_specs=(
            P("dp", None),
            P("dp", None),
            P("dp", None, "fsdp"),
            P("dp", None, "fsdp"),
            P("dp", "fsdp", None),
        ),
        check_vma=False,
    )
```

```python
import functools

import jax
import jax.numpy as jnp
from jax import lax
from jax.experimental import pallas as pl
from jax.experimental.pallas import tpu as pltpu
from jax.sharding import PartitionSpec as P

MESH = pl.DeviceIdType.MESH
NY, NZH, NZ, NX, NC = 4, 2, 4, 4, 2
BF, F32 = jnp.bfloat16, jnp.float32
TRAIL = (((1,), (1,)), ((), ()))
LEAD = (((0,), (0,)), ((), ()))


class Dims:
    def __init__(self, tok, feat, hid):
        self.tok, self.feat, self.hid = tok, feat, hid
        self.cap = tok * 3 // 8
        self.grp = NY * self.cap
        self.quart = feat // NX
        self.half = self.quart // 2
        self.tile = self.quart // 6


def experts_kernel(
    dims,
    routes_hbm, weights_hbm, tokens_hbm, cotangent_hbm, gate_hbm, up_hbm, down_hbm,
    outs, gg, gu, gd,
    routes, weights, mine, first, second, send,
    arr, wg, wu, wd, hid, gdy, udy, tt, dd, rl1, rr1, rl2, rr2, yy, zr, ww, uu,
    ss, rs, ls,
):
    scope = jax.named_scope
    cap, grp, quart, half, tile = dims.cap, dims.grp, dims.quart, dims.half, dims.tile
    dp, fs = lax.axis_index("dp"), lax.axis_index("fsdp")
    y, zh = dp // 2, dp % 2
    z, x, k = fs // 8, (fs // 2) % 4, fs % 2
    other = 1 - k

    def dev(yy_, zh_, z_, x_, k_):
        return (yy_ * 2 + zh_, (z_ * 4 + x_) * 2 + k_)

    def up_y(d):
        return (y + d) % 4

    right, left = dev(y, zh, z, (x + 1) % 4, k), dev(y, zh, z, (x + 3) % 4, k)
    sibling = dev(y, zh, z, x, other)

    used, out_used, drains = [0], [0], []

    def fresh():
        used[0] += 1
        return used[0] - 1

    def group(region=None):
        out_used[0] += 1
        if region is not None:
            drains.append((out_used[0] - 1, region))
        return out_used[0] - 1

    def copy(o, i, src, dst, to):
        return pltpu.make_async_remote_copy(
            src_ref=src, dst_ref=dst, send_sem=ss.at[o], recv_sem=rs.at[i],
            device_id=to, device_id_type=MESH,
        )

    def push(o, i, src, dst, to):
        copy(o, i, src, dst, to).start()

    def got(i, region):
        copy(0, i, region, region, sibling).wait_recv()

    def drained(o, region):
        copy(o, 0, region, region, sibling).wait_send()

    def qcols(q, off=0, width=None):
        return pl.ds(pl.multiple_of(q * quart + off, 128), quart if width is None else width)

    def rows_of(b):
        return pl.ds(pl.multiple_of(b * cap, 16), cap)

    def tcols(t, base=0):
        return pl.ds(pl.multiple_of(base + t * tile, 128), tile)

    barrier = pltpu.get_barrier_semaphore()
    partners = [right, left, sibling]
    for d in range(4):
        partners.append(dev(up_y(d), 1 - zh, z, x, k))
        for turn in range(4):
            if d or turn:
                partners.append(dev(up_y(d), zh, (z + turn) % 4, x, k))
    for p in partners:
        pl.semaphore_signal(barrier, inc=1, device_id=p, device_id_type=MESH)

    tables = [
        pltpu.make_async_copy(routes_hbm, routes, ls.at[4]),
        pltpu.make_async_copy(weights_hbm, weights, ls.at[5]),
    ]
    for c in tables:
        c.start()

    @pl.when(k == 0)
    def _():
        pltpu.make_async_copy(tokens_hbm, mine, ls.at[3]).start()

    @pl.when(k == 1)
    def _():
        pltpu.make_async_copy(cotangent_hbm, mine, ls.at[3]).start()

    loads = [
        pltpu.make_async_copy(s, d, ls.at[n])
        for n, (s, d) in enumerate(((gate_hbm, wg), (up_hbm, wu), (down_hbm, wd)))
    ]
    for c in loads:
        c.start()
    for c in tables:
        c.wait()

    experts = NY * NZH
    seat = lax.broadcasted_iota(jnp.int32, (experts, dims.tok), 0)
    expert = (seat % NY) * NZH + seat // NY
    hit_first = (routes[0:1, :] == expert).astype(F32)
    hit_second = (routes[1:2, :] == expert).astype(F32)
    earlier = (
        lax.broadcasted_iota(jnp.int32, (dims.tok, dims.tok), 0)
        < lax.broadcasted_iota(jnp.int32, (dims.tok, dims.tok), 1)
    ).astype(F32).astype(BF)
    place = jnp.dot(
        (hit_first + hit_second).astype(BF), earlier, preferred_element_type=F32
    )
    slot = lax.broadcasted_iota(jnp.int32, (cap, dims.tok), 0).astype(F32)
    for e in range(experts):
        here = (place[e : e + 1, :] == slot).astype(F32)
        at = pl.ds((e % NY) * cap, cap)
        first[e // NY, at] = (here * hit_first[e : e + 1, :]).astype(BF)
        second[e // NY, at] = (here * hit_second[e : e + 1, :]).astype(BF)

    def fill(g, at):
        f, s = first[g].astype(F32), second[g].astype(F32)
        scale = jnp.sum(f * weights[0:1, :] + s * weights[1:2, :], axis=1, keepdims=True)
        scale = jnp.where(k == 0, jnp.ones_like(scale), scale)
        send[g, :, at] = (
            jnp.dot((f + s).astype(BF), mine[:, at], preferred_element_type=F32) * scale
        ).astype(BF)

    zc = 1 - zh
    pltpu.make_async_copy(tokens_hbm, mine, ls.at[3]).wait()
    with scope("fill_cross"):
        fill(zc, qcols(x))
    with scope("barrier"):
        pl.semaphore_wait(barrier, len(partners))
    ring_order = [(0, 2), (1, 0), (1, 1), (1, 3), (1, 2)]
    send_ids = {b: fresh() for b in ring_order + [(0, 1), (0, 3)]}
    both_ids = [fresh() for _ in range(2)]
    ring = {b: [fresh() for _ in range(3)] for b in ring_order}
    rows5 = pl.ds(0, len(ring_order) * cap // 3)
    fives = arr.at[0, 0, rows5, pl.ds(0, 3 * quart)]
    fives_half = arr.at[0, 0, rows5, pl.ds(0, 3 * half)]
    pair_ids = {d: fresh() for d in range(4)}
    own_half, pair_half = (z % 2) * half, (1 - z % 2) * half
    partner = dev(y, zh, z + 1 - 2 * (z % 2), x, k)
    out_quart = group(send.at[0, pl.ds(0, cap), pl.ds(0, 3 * quart)])
    out_pair = group(arr.at[0, 0, pl.ds(0, cap), pl.ds(0, 2 * quart)])
    out_full = group(send.at[0, pl.ds(0, 2 * cap)])
    out_both = [group(arr.at[0, 0]) for _ in range(2)]
    out_ring = [group(r) for r in (fives, fives, fives_half, fives_half)]
    for d in (0, 1, 3, 2):
        push(
            out_quart, send_ids[1, d],
            send.at[zc, rows_of(up_y(d)), qcols(x, own_half, half)],
            arr.at[k, zh, rows_of(y), qcols(x, own_half, half)],
            dev(up_y(d), zc, z, x, k),
        )
    with scope("fill_same"):
        for q in (x, (x + 1) % 4, (x + 2) % 4, (x + 3) % 4):
            fill(zh, qcols(q))
    push(
        out_quart, send_ids[0, 2],
        send.at[zh, rows_of(up_y(2)), qcols(x)],
        arr.at[k, zh, rows_of(y), qcols(x)],
        dev(up_y(2), zh, z, x, k),
    )
    for d in (1, 3):
        push(
            out_full, send_ids[0, d],
            send.at[zh, rows_of(up_y(d))],
            arr.at[k, zh, rows_of(y)],
            dev(up_y(d), zh, z, x, k),
        )
    push(
        out_both[0], both_ids[0], send.at[zh, rows_of(y)], arr.at[k, zh, rows_of(y)], sibling
    )
    arr[k, zh, rows_of(y)] = send[zh, rows_of(y)]

    def block_of(b, *cols):
        g, d = b
        rows = rows_of(up_y(4 - d) if d else y)
        return arr.at[(k, zc if g else zh, rows) + cols]

    def crossed(d):
        with scope(f"crossed_{d}"):
            part_ = block_of((1, d), qcols(x, own_half, half))
            got(send_ids[1, d], part_)
            push(out_pair, pair_ids[d], part_, part_, partner)

    def ring_one(b):
        with scope(f"ring_one_{b[0]}{b[1]}"):
            near = block_of(b, qcols(x))
            if b[0]:
                got(pair_ids[b[1]], block_of(b, qcols(x, pair_half, half)))
            else:
                got(send_ids[b], near)
            push(out_ring[0], ring[b][0], near, near, right)
            push(out_ring[1], ring[b][1], near, near, left)

    def ring_two(b):
        with scope(f"ring_two_{b[0]}{b[1]}"):
            got(ring[b][0], block_of(b, qcols((x + 3) % 4)))
            near = block_of(b, qcols((x + 3) % 4, 0, half))
            push(out_ring[2], ring[b][2], near, near, right)
            got(ring[b][1], block_of(b, qcols((x + 1) % 4)))
            near = block_of(b, qcols((x + 1) % 4, half, half))
            push(out_ring[3], ring[b][2], near, near, left)

    def ring_end(b):
        with scope(f"ring_end_{b[0]}{b[1]}"):
            got(ring[b][2], block_of(b, qcols((x + 2) % 4)))
            push(out_both[b[0]], both_ids[b[0]], block_of(b), block_of(b), sibling)

    def same_block(d):
        with scope(f"same_block_{d}"):
            got(send_ids[0, d], block_of((0, d)))
            push(out_both[0], both_ids[0], block_of((0, d)), block_of((0, d)), sibling)

    def both_here(g):
        with scope(f"both_here_{g}"):
            got(both_ids[g], arr.at[other, zc if g else zh])

    def first_stage(g):
        zg = zh if g == 0 else zc
        gate_pre = jnp.dot(arr[0, zg], wg[...], preferred_element_type=F32)
        up_pre = jnp.dot(arr[0, zg], wu[...], preferred_element_type=F32)
        hidden_dy = lax.dot_general(arr[1, zg], wd[...], TRAIL, preferred_element_type=F32)
        sigma = jax.nn.sigmoid(gate_pre)
        active = gate_pre * sigma
        hid[zg] = (active * up_pre).astype(BF)
        gdy[zg] = (hidden_dy * up_pre * sigma * (1.0 + gate_pre * (1.0 - sigma))).astype(BF)
        udy[zg] = (hidden_dy * active).astype(BF)

    quarters = [(x + 2) % 4, (x + 1) % 4, (x + 3) % 4, x]
    swap_ids = {(g, n): fresh() for g in range(2) for n in range(4)}
    out_swap = [group(dd.at[g]) for g in range(2)]
    out_hop = {
        (g, n): group(tt.at[g, 0, :, pl.ds(0, 3 * half)]) for g in range(2) for n in range(2)
    }

    parts = (2, 4)
    hop_ids = {(g, h, n): fresh() for g in range(2) for h in range(parts[g]) for n in range(4)}

    def plus(a, b):
        return (a.astype(F32) + b.astype(F32)).astype(BF)

    def rows_h(g, h):
        return pl.ds(h * (grp // parts[g]), grp // parts[g])

    def hop(g, h, n):
        q = quarters[(0, 0, 1, 2, 1, 2)[n]]
        off = (0, half, half, 0, 0, half)[n]
        rows = rows_h(g, h)
        source = tt.at[g, k, rows, qcols(q, off, half)]
        if n < 2:
            target = (rl1, rr1)[n].at[g, rows]
        else:
            target = (rl2 if n % 2 == 0 else rr2).at[g, rows, pl.ds(off, half)]
        push(out_hop[g, n % 2], hop_ids[g, h, n - 2 if n > 3 else n], source, target, right if n % 2 == 0 else left)

    def chip_sum(g, n):
        with scope(f"chip_sum_{g}{n}"):
            q = quarters[n]
            got(swap_ids[g, n], dd.at[g, :, qcols(q)])
            tt[g, k, :, qcols(q)] = plus(tt[g, k, :, qcols(q)], dd[g, :, qcols(q)])
            if n == 0:
                for h in range(parts[g]):
                    hop(g, h, 0)
                    hop(g, h, 1)
            if n in (1, 2):
                hop(g, 0, n + 1)

    def second_part(g, n):
        zg = zh if g == 0 else zc
        width = quart // 3
        q = quarters[n]

        def body(c, carry):
            at = pl.ds(pl.multiple_of(q * quart + c * width, 128), width)
            tt[g, 0, :, at] = jnp.dot(
                hid[zg], wd[:, at], preferred_element_type=F32
            ).astype(BF)
            tt[g, 1, :, at] = (
                lax.dot_general(gdy[zg], wg[at, :], TRAIL, preferred_element_type=F32)
                + lax.dot_general(udy[zg], wu[at, :], TRAIL, preferred_element_type=F32)
            ).astype(BF)
            return carry

        with scope(f"second_{g}{n}"):
            for c in range(3):
                body(c, 0)
        push(
            out_swap[g], swap_ids[g, n], tt.at[g, other, :, qcols(q)], dd.at[g, :, qcols(q)],
            sibling,
        )

    def hop_two(g, h):
        with scope(f"hop_two_{g}{h}"):
            rows = rows_h(g, h)
            got(hop_ids[g, h, 0], rl1.at[g, rows])
            at = qcols(quarters[1], 0, half)
            tt[g, k, rows, at] = plus(tt[g, k, rows, at], rl1[g, rows])
            hop(g, h, 4)
            got(hop_ids[g, h, 1], rr1.at[g, rows])
            at = qcols(quarters[2], half, half)
            tt[g, k, rows, at] = plus(tt[g, k, rows, at], rr1[g, rows])
            hop(g, h, 5)

    def head(zz):
        return (3 * zz + 1 - k) // 2

    def pair(zz):
        return (zz + k) % 2 == 0

    home_ids = [fresh() for _ in range(5)]
    along_ids = {(h, d): fresh() for h in range(parts[1]) for d in range(1, 4)}
    out_home = [group() for _ in range(5)]
    out_along = {d: group() for d in range(1, 4)}

    def home_copy(d, b, wide):
        width = 2 * tile if wide else tile
        zz = (z + d) % 4
        return pltpu.make_async_remote_copy(
            src_ref=yy.at[0, rows_of(b), pl.ds(pl.multiple_of(head(zz) * tile, 128), width)],
            dst_ref=uu.at[zh, d, rows_of(y), pl.ds(0, width)],
            send_sem=ss.at[out_home[d]], recv_sem=rs.at[home_ids[d]],
            device_id=dev(b, zh, zz, x, k), device_id_type=MESH,
        )

    def by_width(zz, action):
        pl.when(pair(zz))(lambda: action(True))
        pl.when(jnp.logical_not(pair(zz)))(lambda: action(False))

    def each_home(b):
        for d in (2, 1, 3, 0):
            zz = (z + d) % 4
            if d == 0:
                pl.when(b != y)(
                    lambda d=d, zz=zz: by_width(zz, lambda wide: home_copy(d, b, wide).start())
                )
            else:
                by_width(zz, lambda wide, d=d: home_copy(d, b, wide).start())

    def along(h):
        rows = rows_h(1, h)
        for d in (2, 1, 3):
            zz = (z + d) % 4

            def go(wide, d=d, zz=zz):
                width = 2 * tile if wide else tile
                push(
                    out_along[d], along_ids[h, d],
                    yy.at[1, rows, pl.ds(pl.multiple_of(head(zz) * tile, 128), width)],
                    zr.at[d - 1, rows, pl.ds(0, width)], dev(y, zh, zz, x, k),
                )

            by_width(zz, go)

    def collect(h):
        def add(wide):
            rows, width = rows_h(1, h), 2 * tile if wide else tile
            for d in range(1, 4):
                got(along_ids[h, d], zr.at[d - 1, rows, pl.ds(0, width)])
            for s in range(2 if wide else 1):
                at = pl.ds(s * tile, tile)
                total = yy[1, rows, tcols(head(z) + s)].astype(F32)
                for d in range(1, 4):
                    total = total + zr[d - 1, rows, at].astype(F32)
                ww[rows, at] = total.astype(BF)
            push(
                out_home[4], home_ids[4], ww.at[rows, pl.ds(0, width)],
                uu.at[zh, 0, rows_of(y), pl.ds(0, width)], dev(h, zc, z, x, k),
            )

        with scope(f"collect_{h}"):
            by_width(z, add)

    def finish(g, h):
        with scope(f"finish_{g}{h}"):
            rows = rows_h(g, h)
            got(hop_ids[g, h, 2], rl2.at[g, rows])
            got(hop_ids[g, h, 3], rr2.at[g, rows])
            yy[g, rows] = (
                tt[g, k, rows, qcols(x)].astype(F32)
                + rl2[g, rows].astype(F32)
                + rr2[g, rows].astype(F32)
            ).astype(BF)
            if g == 1:
                along(h)
                return
            for b in (2 * h, 2 * h + 1):
                each_home(b)

                @pl.when(b == y)
                def _(b=b):
                    def keep(wide):
                        for s in range(2 if wide else 1):
                            uu[zh, 0, rows_of(y), pl.ds(s * tile, tile)] = yy[
                                0, rows_of(b), tcols(head(z) + s)
                            ]

                    by_width(z, keep)

    def wait_home():
        def arrived(wide):
            width = 2 * tile if wide else tile
            for d in range(4):
                rows = grp if d else (NY - 1) * cap
                got(home_ids[d], uu.at[zh, d, pl.ds(0, rows), pl.ds(0, width)])
            got(home_ids[4], uu.at[zc, 0, :, pl.ds(0, width)])

        by_width(z, arrived)

    def weight_grads(begin, end):
        width = 256
        rows = 2 * grp

        def body(c, carry):
            at = pl.ds(pl.multiple_of(c * width, 128), width)
            xs = arr[0, :, :, at].reshape(rows, width)
            ys = arr[1, :, :, at].reshape(rows, width)
            gg[at, :] = lax.dot_general(
                xs, gdy[...].reshape(rows, dims.hid), LEAD, preferred_element_type=F32
            ).astype(BF)
            gu[at, :] = lax.dot_general(
                xs, udy[...].reshape(rows, dims.hid), LEAD, preferred_element_type=F32
            ).astype(BF)
            gd[:, at] = lax.dot_general(
                hid[...].reshape(rows, dims.hid), ys, LEAD, preferred_element_type=F32
            ).astype(BF)
            return carry

        with scope(f"weight_grads_{begin}"):
            lax.fori_loop(begin, end, body, 0)

    ring_one((0, 2))
    crossed(0)
    crossed(1)
    ring_two((0, 2))
    crossed(3)
    ring_one((1, 0))
    crossed(2)
    ring_one((1, 1))
    ring_end((0, 2))
    ring_two((1, 0))
    ring_one((1, 3))
    ring_one((1, 2))
    same_block(1)
    same_block(3)
    ring_two((1, 1))
    with scope("weights_here"):
        for c in loads:
            c.wait()
    both_here(0)
    with scope("first_0"):
        first_stage(0)
    second_part(0, 0)
    ring_two((1, 3))
    ring_end((1, 0))
    ring_two((1, 2))
    second_part(0, 1)
    ring_end((1, 1))
    chip_sum(0, 0)
    second_part(0, 2)
    chip_sum(0, 1)
    second_part(0, 3)
    ring_end((1, 3))
    chip_sum(0, 2)
    ring_end((1, 2))
    chip_sum(0, 3)
    hop_two(0, 0)
    hop(0, 1, 2)
    hop(0, 1, 3)
    both_here(1)
    with scope("first_1"):
        first_stage(1)
    second_part(1, 0)
    hop_two(0, 1)
    second_part(1, 1)
    chip_sum(1, 0)
    second_part(1, 2)
    chip_sum(1, 1)
    second_part(1, 3)
    chip_sum(1, 2)
    finish(0, 0)
    chunks = dims.feat // 256
    weight_grads(0, chunks // 3)
    hop_two(1, 0)
    hop(1, 1, 2)
    hop(1, 1, 3)
    finish(0, 1)
    hop_two(1, 1)
    hop(1, 2, 2)
    hop(1, 2, 3)
    chip_sum(1, 3)
    hop_two(1, 2)
    hop(1, 3, 2)
    hop(1, 3, 3)
    hop_two(1, 3)
    finish(1, 0)
    weight_grads(chunks // 3, chunks // 2)
    finish(1, 1)
    weight_grads(chunks // 2, 2 * chunks // 3)
    finish(1, 2)
    collect(0)
    finish(1, 3)
    collect(1)
    weight_grads(2 * chunks // 3, 5 * chunks // 6)
    collect(2)
    collect(3)
    weight_grads(5 * chunks // 6, chunks)

    @pl.when(jnp.logical_not(pair(z)))
    def _():
        uu[:, :, :, pl.ds(tile, tile)] = jnp.zeros((2, 4, grp, tile), BF)

    with scope("wait_home"):
        wait_home()
    total = uu[zh, 0].astype(F32)
    for d in range(1, 4):
        total = total + uu[zh, d].astype(F32)
    uu[zh, 0] = total.astype(BF)
    slots = uu[:, 0].reshape(2 * grp, 2 * tile)
    same_token = (
        lax.broadcasted_iota(jnp.int32, (dims.tok, dims.tok), 0)
        == lax.broadcasted_iota(jnp.int32, (dims.tok, dims.tok), 1)
    )
    share_first = jnp.sum(
        jnp.where(same_token, weights[0:1, :], 0.0), axis=1, keepdims=True
    )
    share_second = jnp.sum(
        jnp.where(same_token, weights[1:2, :], 0.0), axis=1, keepdims=True
    )
    share_first = jnp.where(k == 0, share_first, jnp.ones_like(share_first))
    share_second = jnp.where(k == 0, share_second, jnp.ones_like(share_second))
    mixed = (
        share_first
        * lax.dot_general(
            first[...].reshape(2 * grp, dims.tok), slots, LEAD, preferred_element_type=F32
        )
        + share_second
        * lax.dot_general(
            second[...].reshape(2 * grp, dims.tok), slots, LEAD, preferred_element_type=F32
        )
    ).astype(BF)
    base = x * quart
    outs[k, :, tcols(head(z), base)] = mixed[:, :tile]

    @pl.when(pair(z))
    def _():
        outs[k, :, tcols(head(z) + 1, base)] = mixed[:, tile:]

    last_ids = {(d, s): fresh() for d in range(1, 4) for s in range(2)}
    to_right = [fresh() for _ in range(6)][0]
    to_left = [fresh() for _ in range(6)][0]
    onward, swap_last = fresh(), fresh()
    out_last = [group(), group()]
    one_quart = outs.at[0, :, pl.ds(0, quart)]
    out_right, out_left, out_onward = (group(one_quart) for _ in range(3))
    out_swap_last = group(outs.at[0])

    def cell(q, t):
        return outs.at[k, :, tcols(t, q * quart)]

    def each_tile(zz, action):
        action(0)
        pl.when(pair(zz))(lambda: action(1))

    def near_x(t):
        push(out_right, to_right + t, cell(x, t), cell(x, t), right)
        push(out_left, to_left + t, cell(x, t), cell(x, t), left)

    def first_out(s):
        t = head(z) + s
        near_x(t)
        for d in (1, 3, 2):
            to = dev(y, zh, (z + d) % 4, x, k)
            push(out_last[s], last_ids[d, s], cell(x, t), cell(x, t), to)

    each_tile(z, first_out)
    with scope("last_z"):
        for d in (1, 3, 2):
            zz = (z + 4 - d) % 4

            def relay(s, d=d, zz=zz):
                t = head(zz) + s
                got(last_ids[d, s], cell(x, t))
                near_x(t)

            each_tile(zz, relay)
    def swap_quarter(q):
        cells = outs.at[k, :, qcols(q)]
        push(out_swap_last, swap_last, cells, cells, sibling)

    swap_quarter(x)
    with scope("last_x"):
        for d in (0, 1, 3, 2):
            zz = (z + 4 - d) % 4

            def onwards(s, zz=zz):
                t = head(zz) + s
                from_left, from_right = cell((x + 3) % 4, t), cell((x + 1) % 4, t)
                got(to_right + t, from_left)

                @pl.when(t < 3)
                def _():
                    push(out_onward, onward, from_left, from_left, right)

                got(to_left + t, from_right)

                @pl.when(t >= 3)
                def _():
                    push(out_onward, onward, from_right, from_right, left)

            each_tile(zz, onwards)
    swap_quarter((x + 3) % 4)
    swap_quarter((x + 1) % 4)
    with scope("last_far"):
        got(onward, outs.at[k, :, qcols((x + 2) % 4)])
    swap_quarter((x + 2) % 4)
    with scope("last_swap"):
        got(swap_last, outs.at[other])
    with scope("drain"):
        for o, region in drains:
            drained(o, region)
        for d in range(4):
            rows = grp if d else (NY - 1) * cap

            def sent_home(wide, d=d, rows=rows):
                width = 2 * tile if wide else tile
                drained(out_home[d], yy.at[0, pl.ds(0, rows), pl.ds(0, width)])
                if d:
                    drained(out_along[d], yy.at[1, :, pl.ds(0, width)])
                else:
                    drained(out_home[4], ww.at[:, pl.ds(0, width)])

            by_width((z + d) % 4, sent_home)
        each_tile(z, lambda s: drained(out_last[s], outs.at[0, :, pl.ds(0, 3 * tile)]))
    assert used[0] == rs.shape[0] and out_used[0] == ss.shape[0], (used, out_used)


def store_kernel(outs, gg, gu, gd, out, dx, gg_hbm, gu_hbm, gd_hbm, sems):
    pairs = ((outs.at[0], out), (outs.at[1], dx), (gg, gg_hbm), (gu, gu_hbm), (gd, gd_hbm))
    copies = [pltpu.make_async_copy(s, d, sems.at[n]) for n, (s, d) in enumerate(pairs)]
    for c in copies:
        c.start()
    for c in copies:
        c.wait()


def on_device(tokens, cotangent, routes, router_weight, w_gate, w_up, w_down):
    dims = Dims(tokens.shape[0], tokens.shape[1], w_gate.shape[2])
    grp, feat, hid = dims.grp, dims.feat, dims.hid
    half, quart, tile = dims.half, dims.quart, dims.tile
    vmem = pl.BlockSpec(memory_space=pltpu.VMEM)
    hbm = pl.BlockSpec(memory_space=pl.ANY)
    whole = jax.ShapeDtypeStruct((dims.tok, feat), BF)
    tall, flat = (feat, hid), (hid, feat)
    results = pl.pallas_call(
        functools.partial(experts_kernel, dims),
        out_shape=(
            pltpu.VMEM((2, dims.tok, feat), BF),
            pltpu.VMEM(tall, BF),
            pltpu.VMEM(tall, BF),
            pltpu.VMEM(flat, BF),
        ),
        in_specs=[hbm] * 7,
        out_specs=(vmem,) * 4,
        scratch_shapes=[
            pltpu.VMEM(routes.T.shape, jnp.int32),
            pltpu.VMEM(routes.T.shape, F32),
            pltpu.VMEM((dims.tok, feat), BF),
            pltpu.VMEM((2, grp, dims.tok), BF),
            pltpu.VMEM((2, grp, dims.tok), BF),
            pltpu.VMEM((2, grp, feat), BF),
            pltpu.VMEM((2, 2, grp, feat), BF),
            pltpu.VMEM((feat, hid), BF),
            pltpu.VMEM((feat, hid), BF),
            pltpu.VMEM((hid, feat), BF),
            pltpu.VMEM((2, grp, hid), BF),
            pltpu.VMEM((2, grp, hid), BF),
            pltpu.VMEM((2, grp, hid), BF),
            pltpu.VMEM((2, 2, grp, feat), BF),
            pltpu.VMEM((2, grp, feat), BF),
            pltpu.VMEM((2, grp, half), BF),
            pltpu.VMEM((2, grp, half), BF),
            pltpu.VMEM((2, grp, quart), BF),
            pltpu.VMEM((2, grp, quart), BF),
            pltpu.VMEM((2, grp, quart), BF),
            pltpu.VMEM((3, grp, 2 * tile), BF),
            pltpu.VMEM((grp, 2 * tile), BF),
            pltpu.VMEM((2, 4, grp, 2 * tile), BF),
            pltpu.SemaphoreType.DMA((29,)),
            pltpu.SemaphoreType.DMA((97,)),
            pltpu.SemaphoreType.DMA((6,)),
        ],
        compiler_params=pltpu.CompilerParams(
            collective_id=0, has_side_effects=True, vmem_limit_bytes=48 * 1024 * 1024
        ),
        name="experts",
    )(routes.T, router_weight.T, tokens, cotangent, w_gate[0], w_up[0], w_down[0])
    output, input_grad, grad_gate, grad_up, grad_down = pl.pallas_call(
        store_kernel,
        out_shape=(
            whole, whole, jax.ShapeDtypeStruct(tall, BF), jax.ShapeDtypeStruct(tall, BF),
            jax.ShapeDtypeStruct(flat, BF),
        ),
        in_specs=[vmem] * 4,
        out_specs=(hbm,) * 5,
        scratch_shapes=[pltpu.SemaphoreType.DMA((5,))],
        compiler_params=pltpu.CompilerParams(vmem_limit_bytes=16 * 1024 * 1024),
        name="store",
    )(*(pltpu.with_memory_space_constraint(r, pltpu.VMEM) for r in results))
    return (output, input_grad, grad_gate[None], grad_up[None], grad_down[None])


def solution(mesh):
    return jax.shard_map(
        on_device,
        mesh=mesh,
        in_specs=(
            P("dp", None),
            P("dp", None),
            P("dp", None),
            P("dp", None),
            P("dp", None, "fsdp"),
            P("dp", None, "fsdp"),
            P("dp", "fsdp", None),
        ),
        out_specs=(
            P("dp", None),
            P("dp", None),
            P("dp", None, "fsdp"),
            P("dp", None, "fsdp"),
            P("dp", "fsdp", None),
        ),
        check_vma=False,
    )
```

```python
import functools

import jax
import jax.numpy as jnp
from jax import lax
from jax.experimental import pallas as pl
from jax.experimental.pallas import tpu as pltpu
from jax.sharding import PartitionSpec as P

MESH = pl.DeviceIdType.MESH
NY, NZH, NZ, NX, NC = 4, 2, 4, 4, 2
BF, F32 = jnp.bfloat16, jnp.float32
TRAIL = (((1,), (1,)), ((), ()))
LEAD = (((0,), (0,)), ((), ()))


class Dims:
    def __init__(self, tok, feat, hid):
        self.tok, self.feat, self.hid = tok, feat, hid
        self.cap = tok * 3 // 8
        self.grp = NY * self.cap
        self.quart = feat // NX
        self.half = self.quart // 2
        self.tile = self.quart // 6


def experts_kernel(
    dims,
    routes_hbm, weights_hbm, tokens_hbm, cotangent_hbm, gate_hbm, up_hbm, down_hbm,
    outs, gg, gu, gd,
    routes, weights, mine, first, second, send,
    arr, wg, wu, wd, hid, gdy, udy, tt, dd, near, last, yy, zr, ww, uu,
    ss, rs, ls,
):
    scope = jax.named_scope
    cap, grp, quart, half, tile = dims.cap, dims.grp, dims.quart, dims.half, dims.tile
    dp, fs = lax.axis_index("dp"), lax.axis_index("fsdp")
    y, zh = dp // 2, dp % 2
    z, x, k = fs // 8, (fs // 2) % 4, fs % 2
    other = 1 - k

    def dev(yy_, zh_, z_, x_, k_):
        return (yy_ * 2 + zh_, (z_ * 4 + x_) * 2 + k_)

    def up_y(d):
        return (y + d) % 4

    right, left = dev(y, zh, z, (x + 1) % 4, k), dev(y, zh, z, (x + 3) % 4, k)
    sibling = dev(y, zh, z, x, other)

    used, out_used, drains = [0], [0], []

    def fresh():
        used[0] += 1
        return used[0] - 1

    def group(region=None):
        out_used[0] += 1
        if region is not None:
            drains.append((out_used[0] - 1, region))
        return out_used[0] - 1

    def copy(o, i, src, dst, to):
        return pltpu.make_async_remote_copy(
            src_ref=src, dst_ref=dst, send_sem=ss.at[o], recv_sem=rs.at[i],
            device_id=to, device_id_type=MESH,
        )

    def push(o, i, src, dst, to):
        copy(o, i, src, dst, to).start()

    def got(i, region):
        copy(0, i, region, region, sibling).wait_recv()

    def drained(o, region):
        copy(o, 0, region, region, sibling).wait_send()

    def qcols(q, off=0, width=None):
        return pl.ds(pl.multiple_of(q * quart + off, 128), quart if width is None else width)

    def rows_of(b):
        return pl.ds(pl.multiple_of(b * cap, 16), cap)

    def tcols(t, base=0):
        return pl.ds(pl.multiple_of(base + t * tile, 128), tile)

    barrier = pltpu.get_barrier_semaphore()
    partners = [right, left, sibling]
    for d in range(4):
        partners.append(dev(up_y(d), 1 - zh, z, x, k))
        for turn in range(4):
            if d or turn:
                partners.append(dev(up_y(d), zh, (z + turn) % 4, x, k))
    for p in partners:
        pl.semaphore_signal(barrier, inc=1, device_id=p, device_id_type=MESH)

    tables = [
        pltpu.make_async_copy(routes_hbm, routes, ls.at[4]),
        pltpu.make_async_copy(weights_hbm, weights, ls.at[5]),
    ]
    for c in tables:
        c.start()

    @pl.when(k == 0)
    def _():
        pltpu.make_async_copy(tokens_hbm, mine, ls.at[3]).start()

    @pl.when(k == 1)
    def _():
        pltpu.make_async_copy(cotangent_hbm, mine, ls.at[3]).start()

    loads = [
        pltpu.make_async_copy(s, d, ls.at[n])
        for n, (s, d) in enumerate(((gate_hbm, wg), (up_hbm, wu), (down_hbm, wd)))
    ]
    for c in loads:
        c.start()
    for c in tables:
        c.wait()

    experts = NY * NZH
    seat = lax.broadcasted_iota(jnp.int32, (experts, dims.tok), 0)
    expert = (seat % NY) * NZH + seat // NY
    hit_first = (routes[0:1, :] == expert).astype(F32)
    hit_second = (routes[1:2, :] == expert).astype(F32)
    earlier = (
        lax.broadcasted_iota(jnp.int32, (dims.tok, dims.tok), 0)
        < lax.broadcasted_iota(jnp.int32, (dims.tok, dims.tok), 1)
    ).astype(F32).astype(BF)
    place = jnp.dot(
        (hit_first + hit_second).astype(BF), earlier, preferred_element_type=F32
    )
    slot = lax.broadcasted_iota(jnp.int32, (cap, dims.tok), 0).astype(F32)
    for e in range(experts):
        here = (place[e : e + 1, :] == slot).astype(F32)
        at = pl.ds((e % NY) * cap, cap)
        first[e // NY, at] = (here * hit_first[e : e + 1, :]).astype(BF)
        second[e // NY, at] = (here * hit_second[e : e + 1, :]).astype(BF)

    def fill(g, at):
        f, s = first[g].astype(F32), second[g].astype(F32)
        scale = jnp.sum(f * weights[0:1, :] + s * weights[1:2, :], axis=1, keepdims=True)
        scale = jnp.where(k == 0, jnp.ones_like(scale), scale)
        send[g, :, at] = (
            jnp.dot((f + s).astype(BF), mine[:, at], preferred_element_type=F32) * scale
        ).astype(BF)

    zc = 1 - zh
    pltpu.make_async_copy(tokens_hbm, mine, ls.at[3]).wait()
    with scope("fill_cross"):
        fill(zc, qcols(x))
    with scope("barrier"):
        pl.semaphore_wait(barrier, len(partners))
    ring_order = [(0, 2), (1, 0), (1, 1), (1, 3), (1, 2)]
    send_ids = {b: fresh() for b in ring_order + [(0, 1), (0, 3)]}
    both_ids = [fresh() for _ in range(2)]
    ring = {b: [fresh() for _ in range(3)] for b in ring_order}
    rows5 = pl.ds(0, len(ring_order) * cap // 3)
    fives = arr.at[0, 0, rows5, pl.ds(0, 3 * quart)]
    fives_half = arr.at[0, 0, rows5, pl.ds(0, 3 * half)]
    pair_ids = {d: fresh() for d in range(4)}
    own_half, pair_half = (z % 2) * half, (1 - z % 2) * half
    partner = dev(y, zh, z + 1 - 2 * (z % 2), x, k)
    out_quart = group(send.at[0, pl.ds(0, cap), pl.ds(0, 3 * quart)])
    out_pair = group(arr.at[0, 0, pl.ds(0, cap), pl.ds(0, 2 * quart)])
    out_full = group(send.at[0, pl.ds(0, 2 * cap)])
    out_both = [group(arr.at[0, 0]) for _ in range(2)]
    out_ring = [group(r) for r in (fives, fives, fives_half, fives_half)]
    for d in (0, 1, 3, 2):
        push(
            out_quart, send_ids[1, d],
            send.at[zc, rows_of(up_y(d)), qcols(x, own_half, half)],
            arr.at[k, zh, rows_of(y), qcols(x, own_half, half)],
            dev(up_y(d), zc, z, x, k),
        )
    with scope("fill_same"):
        for q in (x, (x + 1) % 4, (x + 2) % 4, (x + 3) % 4):
            fill(zh, qcols(q))
    push(
        out_quart, send_ids[0, 2],
        send.at[zh, rows_of(up_y(2)), qcols(x)],
        arr.at[k, zh, rows_of(y), qcols(x)],
        dev(up_y(2), zh, z, x, k),
    )
    for d in (1, 3):
        push(
            out_full, send_ids[0, d],
            send.at[zh, rows_of(up_y(d))],
            arr.at[k, zh, rows_of(y)],
            dev(up_y(d), zh, z, x, k),
        )
    push(
        out_both[0], both_ids[0], send.at[zh, rows_of(y)], arr.at[k, zh, rows_of(y)], sibling
    )
    arr[k, zh, rows_of(y)] = send[zh, rows_of(y)]

    def block_of(b, *cols):
        g, d = b
        rows = rows_of(up_y(4 - d) if d else y)
        return arr.at[(k, zc if g else zh, rows) + cols]

    def crossed(d):
        with scope(f"crossed_{d}"):
            part_ = block_of((1, d), qcols(x, own_half, half))
            got(send_ids[1, d], part_)
            push(out_pair, pair_ids[d], part_, part_, partner)

    def ring_one(b):
        with scope(f"ring_one_{b[0]}{b[1]}"):
            near = block_of(b, qcols(x))
            if b[0]:
                got(pair_ids[b[1]], block_of(b, qcols(x, pair_half, half)))
            else:
                got(send_ids[b], near)
            push(out_ring[0], ring[b][0], near, near, right)
            push(out_ring[1], ring[b][1], near, near, left)

    def ring_two(b):
        with scope(f"ring_two_{b[0]}{b[1]}"):
            got(ring[b][0], block_of(b, qcols((x + 3) % 4)))
            near = block_of(b, qcols((x + 3) % 4, 0, half))
            push(out_ring[2], ring[b][2], near, near, right)
            got(ring[b][1], block_of(b, qcols((x + 1) % 4)))
            near = block_of(b, qcols((x + 1) % 4, half, half))
            push(out_ring[3], ring[b][2], near, near, left)

    def ring_end(b):
        with scope(f"ring_end_{b[0]}{b[1]}"):
            got(ring[b][2], block_of(b, qcols((x + 2) % 4)))
            push(out_both[b[0]], both_ids[b[0]], block_of(b), block_of(b), sibling)

    def same_block(d):
        with scope(f"same_block_{d}"):
            got(send_ids[0, d], block_of((0, d)))
            push(out_both[0], both_ids[0], block_of((0, d)), block_of((0, d)), sibling)

    def both_here(g):
        with scope(f"both_here_{g}"):
            got(both_ids[g], arr.at[other, zc if g else zh])

    def first_stage(g):
        zg = zh if g == 0 else zc
        gate_pre = jnp.dot(arr[0, zg], wg[...], preferred_element_type=F32)
        up_pre = jnp.dot(arr[0, zg], wu[...], preferred_element_type=F32)
        hidden_dy = lax.dot_general(arr[1, zg], wd[...], TRAIL, preferred_element_type=F32)
        sigma = jax.nn.sigmoid(gate_pre)
        active = gate_pre * sigma
        hid[zg] = (active * up_pre).astype(BF)
        gdy[zg] = (hidden_dy * up_pre * sigma * (1.0 + gate_pre * (1.0 - sigma))).astype(BF)
        udy[zg] = (hidden_dy * active).astype(BF)

    quarters = [(x + 2) % 4, (x + 1) % 4, (x + 3) % 4, x]
    swap_ids = {(g, n): fresh() for g in range(2) for n in range(4)}
    out_swap = [group(dd.at[g]) for g in range(2)]
    out_hop = {
        (g, n): group(tt.at[g, 0, :, pl.ds(0, 3 * half)]) for g in range(2) for n in range(2)
    }

    parts = (2, 4)
    hop_ids = {(g, h, n): fresh() for g in range(2) for h in range(parts[g]) for n in range(2)}

    def plus(a, b):
        return (a.astype(F32) + b.astype(F32)).astype(BF)

    def rows_h(g, h):
        return pl.ds(h * (grp // parts[g]), grp // parts[g])

    def hop(g, h, n):
        q = quarters[(0, 0, 1, 2, 1, 2)[n]]
        off = (0, half, half, 0, 0, half)[n]
        rows = rows_h(g, h)
        source = tt.at[g, k, rows, qcols(q, off, half)]
        if n < 2:
            target = near.at[g, rows, pl.ds(n * half, half)]
        else:
            target = last.at[g, rows, pl.ds((n % 2) * quart + off, half)]
        push(out_hop[g, n % 2], hop_ids[g, h, 0 if n < 2 else 1], source, target, right if n % 2 == 0 else left)

    def chip_sum(g, n):
        with scope(f"chip_sum_{g}{n}"):
            q = quarters[n]
            got(swap_ids[g, n], dd.at[g, :, qcols(q)])
            tt[g, k, :, qcols(q)] = plus(tt[g, k, :, qcols(q)], dd[g, :, qcols(q)])
            if n == 0:
                for h in range(parts[g]):
                    hop(g, h, 0)
                    hop(g, h, 1)
            if n in (1, 2):
                hop(g, 0, n + 1)

    def second_part(g, n):
        zg = zh if g == 0 else zc
        width = quart // 3
        q = quarters[n]

        def body(c, carry):
            at = pl.ds(pl.multiple_of(q * quart + c * width, 128), width)
            tt[g, 0, :, at] = jnp.dot(
                hid[zg], wd[:, at], preferred_element_type=F32
            ).astype(BF)
            tt[g, 1, :, at] = (
                lax.dot_general(gdy[zg], wg[at, :], TRAIL, preferred_element_type=F32)
                + lax.dot_general(udy[zg], wu[at, :], TRAIL, preferred_element_type=F32)
            ).astype(BF)
            return carry

        with scope(f"second_{g}{n}"):
            for c in range(3):
                body(c, 0)
        push(
            out_swap[g], swap_ids[g, n], tt.at[g, other, :, qcols(q)], dd.at[g, :, qcols(q)],
            sibling,
        )

    def hop_two(g, h):
        with scope(f"hop_two_{g}{h}"):
            rows = rows_h(g, h)
            got(hop_ids[g, h, 0], near.at[g, rows])
            at = qcols(quarters[1], 0, half)
            tt[g, k, rows, at] = plus(tt[g, k, rows, at], near[g, rows, :half])
            hop(g, h, 4)
            at = qcols(quarters[2], half, half)
            tt[g, k, rows, at] = plus(tt[g, k, rows, at], near[g, rows, half:])
            hop(g, h, 5)

    def head(zz):
        return (3 * zz + 1 - k) // 2

    def pair(zz):
        return (zz + k) % 2 == 0

    home_ids = [fresh() for _ in range(5)]
    along_ids = [fresh() for _ in range(parts[1])]
    out_home = [group() for _ in range(5)]
    out_along = {d: group() for d in range(1, 4)}

    def home_copy(d, b, wide):
        width = 2 * tile if wide else tile
        zz = (z + d) % 4
        return pltpu.make_async_remote_copy(
            src_ref=yy.at[0, rows_of(b), pl.ds(pl.multiple_of(head(zz) * tile, 128), width)],
            dst_ref=uu.at[zh, d, rows_of(y), pl.ds(0, width)],
            send_sem=ss.at[out_home[d]], recv_sem=rs.at[home_ids[d]],
            device_id=dev(b, zh, zz, x, k), device_id_type=MESH,
        )

    def by_width(zz, action):
        pl.when(pair(zz))(lambda: action(True))
        pl.when(jnp.logical_not(pair(zz)))(lambda: action(False))

    def each_home(b):
        for d in (2, 1, 3, 0):
            zz = (z + d) % 4
            if d == 0:
                pl.when(b != y)(
                    lambda d=d, zz=zz: by_width(zz, lambda wide: home_copy(d, b, wide).start())
                )
            else:
                by_width(zz, lambda wide, d=d: home_copy(d, b, wide).start())

    def along(h):
        rows = rows_h(1, h)
        for d in (2, 1, 3):
            zz = (z + d) % 4

            def go(wide, d=d, zz=zz):
                width = 2 * tile if wide else tile
                push(
                    out_along[d], along_ids[h],
                    yy.at[1, rows, pl.ds(pl.multiple_of(head(zz) * tile, 128), width)],
                    zr.at[d - 1, rows, pl.ds(0, width)], dev(y, zh, zz, x, k),
                )

            by_width(zz, go)

    def collect(h):
        def add(wide):
            rows, width = rows_h(1, h), 2 * tile if wide else tile
            got(along_ids[h], zr.at[:, rows, pl.ds(0, width)])
            for s in range(2 if wide else 1):
                at = pl.ds(s * tile, tile)
                total = yy[1, rows, tcols(head(z) + s)].astype(F32)
                for d in range(1, 4):
                    total = total + zr[d - 1, rows, at].astype(F32)
                ww[rows, at] = total.astype(BF)
            push(
                out_home[4], home_ids[4], ww.at[rows, pl.ds(0, width)],
                uu.at[zh, 0, rows_of(y), pl.ds(0, width)], dev(h, zc, z, x, k),
            )

        with scope(f"collect_{h}"):
            by_width(z, add)

    def finish(g, h):
        with scope(f"finish_{g}{h}"):
            rows = rows_h(g, h)
            got(hop_ids[g, h, 1], last.at[g, rows])
            yy[g, rows] = (
                tt[g, k, rows, qcols(x)].astype(F32)
                + last[g, rows, :quart].astype(F32)
                + last[g, rows, quart:].astype(F32)
            ).astype(BF)
            if g == 1:
                along(h)
                return
            for b in (2 * h, 2 * h + 1):
                each_home(b)

                @pl.when(b == y)
                def _(b=b):
                    def keep(wide):
                        for s in range(2 if wide else 1):
                            uu[zh, 0, rows_of(y), pl.ds(s * tile, tile)] = yy[
                                0, rows_of(b), tcols(head(z) + s)
                            ]

                    by_width(z, keep)

    def wait_home():
        def arrived(wide):
            width = 2 * tile if wide else tile
            for d in range(4):
                rows = grp if d else (NY - 1) * cap
                got(home_ids[d], uu.at[zh, d, pl.ds(0, rows), pl.ds(0, width)])
            got(home_ids[4], uu.at[zc, 0, :, pl.ds(0, width)])

        by_width(z, arrived)

    def weight_grads(begin, end):
        width = 256
        rows = 2 * grp

        def body(c, carry):
            at = pl.ds(pl.multiple_of(c * width, 128), width)
            xs = arr[0, :, :, at].reshape(rows, width)
            ys = arr[1, :, :, at].reshape(rows, width)
            gg[at, :] = lax.dot_general(
                xs, gdy[...].reshape(rows, dims.hid), LEAD, preferred_element_type=F32
            ).astype(BF)
            gu[at, :] = lax.dot_general(
                xs, udy[...].reshape(rows, dims.hid), LEAD, preferred_element_type=F32
            ).astype(BF)
            gd[:, at] = lax.dot_general(
                hid[...].reshape(rows, dims.hid), ys, LEAD, preferred_element_type=F32
            ).astype(BF)
            return carry

        with scope(f"weight_grads_{begin}"):
            lax.fori_loop(begin, end, body, 0)

    ring_one((0, 2))
    crossed(0)
    crossed(1)
    ring_two((0, 2))
    crossed(3)
    ring_one((1, 0))
    crossed(2)
    ring_one((1, 1))
    ring_end((0, 2))
    ring_two((1, 0))
    ring_one((1, 3))
    ring_one((1, 2))
    same_block(1)
    same_block(3)
    ring_two((1, 1))
    with scope("weights_here"):
        for c in loads:
            c.wait()
    both_here(0)
    with scope("first_0"):
        first_stage(0)
    second_part(0, 0)
    ring_two((1, 3))
    ring_end((1, 0))
    ring_two((1, 2))
    second_part(0, 1)
    ring_end((1, 1))
    chip_sum(0, 0)
    second_part(0, 2)
    chip_sum(0, 1)
    second_part(0, 3)
    ring_end((1, 3))
    chip_sum(0, 2)
    ring_end((1, 2))
    chip_sum(0, 3)
    hop_two(0, 0)
    hop(0, 1, 2)
    hop(0, 1, 3)
    both_here(1)
    with scope("first_1"):
        first_stage(1)
    second_part(1, 0)
    hop_two(0, 1)
    second_part(1, 1)
    chip_sum(1, 0)
    second_part(1, 2)
    chip_sum(1, 1)
    second_part(1, 3)
    chip_sum(1, 2)
    finish(0, 0)
    chunks = dims.feat // 256
    weight_grads(0, chunks // 3)
    hop_two(1, 0)
    hop(1, 1, 2)
    hop(1, 1, 3)
    finish(0, 1)
    hop_two(1, 1)
    hop(1, 2, 2)
    hop(1, 2, 3)
    chip_sum(1, 3)
    hop_two(1, 2)
    hop(1, 3, 2)
    hop(1, 3, 3)
    hop_two(1, 3)
    finish(1, 0)
    weight_grads(chunks // 3, chunks // 2)
    finish(1, 1)
    weight_grads(chunks // 2, 2 * chunks // 3)
    finish(1, 2)
    collect(0)
    finish(1, 3)
    collect(1)
    weight_grads(2 * chunks // 3, 5 * chunks // 6)
    collect(2)
    collect(3)
    weight_grads(5 * chunks // 6, chunks)

    @pl.when(jnp.logical_not(pair(z)))
    def _():
        uu[:, :, :, pl.ds(tile, tile)] = jnp.zeros((2, 4, grp, tile), BF)

    with scope("wait_home"):
        wait_home()
    total = uu[zh, 0].astype(F32)
    for d in range(1, 4):
        total = total + uu[zh, d].astype(F32)
    uu[zh, 0] = total.astype(BF)
    slots = uu[:, 0].reshape(2 * grp, 2 * tile)
    same_token = (
        lax.broadcasted_iota(jnp.int32, (dims.tok, dims.tok), 0)
        == lax.broadcasted_iota(jnp.int32, (dims.tok, dims.tok), 1)
    )
    share_first = jnp.sum(
        jnp.where(same_token, weights[0:1, :], 0.0), axis=1, keepdims=True
    )
    share_second = jnp.sum(
        jnp.where(same_token, weights[1:2, :], 0.0), axis=1, keepdims=True
    )
    share_first = jnp.where(k == 0, share_first, jnp.ones_like(share_first))
    share_second = jnp.where(k == 0, share_second, jnp.ones_like(share_second))
    mixed = (
        share_first
        * lax.dot_general(
            first[...].reshape(2 * grp, dims.tok), slots, LEAD, preferred_element_type=F32
        )
        + share_second
        * lax.dot_general(
            second[...].reshape(2 * grp, dims.tok), slots, LEAD, preferred_element_type=F32
        )
    ).astype(BF)
    base = x * quart
    outs[k, :, tcols(head(z), base)] = mixed[:, :tile]

    @pl.when(pair(z))
    def _():
        outs[k, :, tcols(head(z) + 1, base)] = mixed[:, tile:]

    last_ids = {(d, s): fresh() for d in range(1, 4) for s in range(2)}
    to_right = [fresh() for _ in range(6)][0]
    to_left = [fresh() for _ in range(6)][0]
    onward, swap_last = fresh(), fresh()
    out_last = [group(), group()]
    one_quart = outs.at[0, :, pl.ds(0, quart)]
    out_right, out_left, out_onward = (group(one_quart) for _ in range(3))
    out_swap_last = group(outs.at[0])

    def cell(q, t):
        return outs.at[k, :, tcols(t, q * quart)]

    def each_tile(zz, action):
        action(0)
        pl.when(pair(zz))(lambda: action(1))

    def near_x(t):
        push(out_right, to_right + t, cell(x, t), cell(x, t), right)
        push(out_left, to_left + t, cell(x, t), cell(x, t), left)

    def first_out(s):
        t = head(z) + s
        near_x(t)
        for d in (1, 3, 2):
            to = dev(y, zh, (z + d) % 4, x, k)
            push(out_last[s], last_ids[d, s], cell(x, t), cell(x, t), to)

    each_tile(z, first_out)
    with scope("last_z"):
        for d in (1, 3, 2):
            zz = (z + 4 - d) % 4

            def relay(s, d=d, zz=zz):
                t = head(zz) + s
                got(last_ids[d, s], cell(x, t))
                near_x(t)

            each_tile(zz, relay)
    def swap_quarter(q):
        cells = outs.at[k, :, qcols(q)]
        push(out_swap_last, swap_last, cells, cells, sibling)

    swap_quarter(x)
    with scope("last_x"):
        for d in (0, 1, 3, 2):
            zz = (z + 4 - d) % 4

            def onwards(s, zz=zz):
                t = head(zz) + s
                from_left, from_right = cell((x + 3) % 4, t), cell((x + 1) % 4, t)
                got(to_right + t, from_left)

                @pl.when(t < 3)
                def _():
                    push(out_onward, onward, from_left, from_left, right)

                got(to_left + t, from_right)

                @pl.when(t >= 3)
                def _():
                    push(out_onward, onward, from_right, from_right, left)

            each_tile(zz, onwards)
    swap_quarter((x + 3) % 4)
    swap_quarter((x + 1) % 4)
    with scope("last_far"):
        got(onward, outs.at[k, :, qcols((x + 2) % 4)])
    swap_quarter((x + 2) % 4)
    with scope("last_swap"):
        got(swap_last, outs.at[other])
    with scope("drain"):
        for o, region in drains:
            drained(o, region)
        for d in range(4):
            rows = grp if d else (NY - 1) * cap

            def sent_home(wide, d=d, rows=rows):
                width = 2 * tile if wide else tile
                drained(out_home[d], yy.at[0, pl.ds(0, rows), pl.ds(0, width)])
                if d:
                    drained(out_along[d], yy.at[1, :, pl.ds(0, width)])
                else:
                    drained(out_home[4], ww.at[:, pl.ds(0, width)])

            by_width((z + d) % 4, sent_home)
        each_tile(z, lambda s: drained(out_last[s], outs.at[0, :, pl.ds(0, 3 * tile)]))
    assert used[0] == rs.shape[0] and out_used[0] == ss.shape[0], (used, out_used)


def store_kernel(outs, gg, gu, gd, out, dx, gg_hbm, gu_hbm, gd_hbm, sems):
    pairs = ((outs.at[0], out), (outs.at[1], dx), (gg, gg_hbm), (gu, gu_hbm), (gd, gd_hbm))
    copies = [pltpu.make_async_copy(s, d, sems.at[n]) for n, (s, d) in enumerate(pairs)]
    for c in copies:
        c.start()
    for c in copies:
        c.wait()


def on_device(tokens, cotangent, routes, router_weight, w_gate, w_up, w_down):
    dims = Dims(tokens.shape[0], tokens.shape[1], w_gate.shape[2])
    grp, feat, hid = dims.grp, dims.feat, dims.hid
    half, quart, tile = dims.half, dims.quart, dims.tile
    vmem = pl.BlockSpec(memory_space=pltpu.VMEM)
    hbm = pl.BlockSpec(memory_space=pl.ANY)
    whole = jax.ShapeDtypeStruct((dims.tok, feat), BF)
    tall, flat = (feat, hid), (hid, feat)
    results = pl.pallas_call(
        functools.partial(experts_kernel, dims),
        out_shape=(
            pltpu.VMEM((2, dims.tok, feat), BF),
            pltpu.VMEM(tall, BF),
            pltpu.VMEM(tall, BF),
            pltpu.VMEM(flat, BF),
        ),
        in_specs=[hbm] * 7,
        out_specs=(vmem,) * 4,
        scratch_shapes=[
            pltpu.VMEM(routes.T.shape, jnp.int32),
            pltpu.VMEM(routes.T.shape, F32),
            pltpu.VMEM((dims.tok, feat), BF),
            pltpu.VMEM((2, grp, dims.tok), BF),
            pltpu.VMEM((2, grp, dims.tok), BF),
            pltpu.VMEM((2, grp, feat), BF),
            pltpu.VMEM((2, 2, grp, feat), BF),
            pltpu.VMEM((feat, hid), BF),
            pltpu.VMEM((feat, hid), BF),
            pltpu.VMEM((hid, feat), BF),
            pltpu.VMEM((2, grp, hid), BF),
            pltpu.VMEM((2, grp, hid), BF),
            pltpu.VMEM((2, grp, hid), BF),
            pltpu.VMEM((2, 2, grp, feat), BF),
            pltpu.VMEM((2, grp, feat), BF),
            pltpu.VMEM((2, grp, quart), BF),
            pltpu.VMEM((2, grp, 2 * quart), BF),
            pltpu.VMEM((2, grp, quart), BF),
            pltpu.VMEM((3, grp, 2 * tile), BF),
            pltpu.VMEM((grp, 2 * tile), BF),
            pltpu.VMEM((2, 4, grp, 2 * tile), BF),
            pltpu.SemaphoreType.DMA((29,)),
            pltpu.SemaphoreType.DMA((77,)),
            pltpu.SemaphoreType.DMA((6,)),
        ],
        compiler_params=pltpu.CompilerParams(
            collective_id=0, has_side_effects=True, vmem_limit_bytes=48 * 1024 * 1024
        ),
        name="experts",
    )(routes.T, router_weight.T, tokens, cotangent, w_gate[0], w_up[0], w_down[0])
    output, input_grad, grad_gate, grad_up, grad_down = pl.pallas_call(
        store_kernel,
        out_shape=(
            whole, whole, jax.ShapeDtypeStruct(tall, BF), jax.ShapeDtypeStruct(tall, BF),
            jax.ShapeDtypeStruct(flat, BF),
        ),
        in_specs=[vmem] * 4,
        out_specs=(hbm,) * 5,
        scratch_shapes=[pltpu.SemaphoreType.DMA((5,))],
        compiler_params=pltpu.CompilerParams(vmem_limit_bytes=16 * 1024 * 1024),
        name="store",
    )(*(pltpu.with_memory_space_constraint(r, pltpu.VMEM) for r in results))
    return (output, input_grad, grad_gate[None], grad_up[None], grad_down[None])


def solution(mesh):
    return jax.shard_map(
        on_device,
        mesh=mesh,
        in_specs=(
            P("dp", None),
            P("dp", None),
            P("dp", None),
            P("dp", None),
            P("dp", None, "fsdp"),
            P("dp", None, "fsdp"),
            P("dp", "fsdp", None),
        ),
        out_specs=(
            P("dp", None),
            P("dp", None),
            P("dp", None, "fsdp"),
            P("dp", None, "fsdp"),
            P("dp", "fsdp", None),
        ),
        check_vma=False,
    )
```
